256 devices in a mesh: dp: 16 (over x_lo, y, core), tp: 16 (over z, x_hi).
Axes of the slice: x: 4 (x_hi: 2, x_lo: 2; x = x_hi * 2 + x_lo), y: 4, z: 8, core: 2. Of those that a mesh axis runs over, the one named last changes fastest.
Arguments:
- inputs: bfloat16 [16, 3072, 1280], P('dp', 'tp'), may hold values from -6 to 6
- saved_hidden: bfloat16 [16, 3072, 5120], P('dp', None, 'tp'), may hold values from -8 to 8
- upstream: bfloat16 [16, 3072, 1280], P('dp', 'tp'), may hold values from -6 to 6
- w_in: bfloat16 [1280, 5120], P(None, 'tp'), may hold values from -0.15625 to 0.15625
- w_out: bfloat16 [5120, 1280], P('tp'), may hold values from -0.078125 to 0.078125
- kernel: float32 [7, 1280], replicated, may hold values from -2 to 2
Outputs:
- grad_inputs: bfloat16 [16, 3072, 1280], P('dp', 'tp')
- grad_w_in: float32 [1280, 5120], P(None, 'tp')
- grad_w_out: float32 [5120, 1280], P('tp')
- grad_bias: float32 [5120], P('tp')
- grad_kernel: float32 [7, 1280], replicated
The draws below stay inside these ranges and needn't reach their ends.
All inputs are finite; a program needn't handle non-finite values.
Results may differ from the reference program's by a relative error of at most 0.02.
Values may be sent and summed in bfloat16 or wider, within the bound.
A program may use at most 128 MiB of HBM per device.

```python
from functools import partial
import jax
import jax.numpy as jnp
from jax import lax

D = 1280
FF = 5120
KW = 7
SEQ = 3072
SEQS = 16
N_TP = 16


def shard_levels(stream_key, dims, pieces, low, top_value):
    gain = 1.0
    for position, blocks in pieces:
        draws = jax.random.uniform(jax.random.fold_in(jax.random.fold_in(stream_key, 6), position), (blocks,), jnp.float32, low / len(pieces), top_value / len(pieces))
        gain = gain * jnp.repeat(jnp.exp(draws), dims[position] // blocks).reshape((-1,) + (1,) * (len(dims) - 1 - position))
    return gain


def normal_values(rng, dims, width, reach, split=(), dtype=jnp.bfloat16):
    values = width * jax.random.normal(rng, dims, jnp.float32)
    if split:
        values = values * shard_levels(rng, dims, split, -0.22, 0.18)
    return jnp.clip(values, -reach, reach).astype(dtype)


def setup_inputs(seed: int = 0) -> dict:
    key_of = jax.random.split(jax.random.key(seed), 7)
    return {
        "inputs": normal_values(key_of[0], (SEQS, SEQ, D), 1.0, 6.0, ((0, 16), (1, 16))),
        "saved_hidden": normal_values(key_of[1], (SEQS, SEQ, FF), 1.5, 8.0, ((0, 16), (2, 16))),
        "upstream": normal_values(key_of[2], (SEQS, SEQ, D), 1.0, 6.0, ((0, 16), (1, 16))),
        "w_in": normal_values(key_of[3], (D, FF), D ** -0.5, 0.15625, ((1, 16),)),
        "w_out": normal_values(key_of[4], (FF, D), FF ** -0.5, 0.078125, ((0, 16),)),
        "kernel": normal_values(key_of[5], (KW, D), 0.3, 2.0, (), jnp.float32),
    }


def gelu_exact(value):
    return jax.nn.gelu(value, approximate=False)

def one_sequence(carry, items, w_in, w_out, kernel):
    total_in, total_out, total_bias, total_kernel = carry
    inputs, hidden, upstream = items
    length = inputs.shape[0]
    inputs_f = inputs.astype(jnp.float32)
    padded = jnp.pad(inputs_f, ((3, 3), (0, 0)))
    mixed = inputs_f
    for tap in range(KW):
        mixed = mixed + kernel[tap] * padded[tap:tap + length]
    mixed = mixed.astype(jnp.bfloat16)
    hidden_f = hidden.astype(jnp.float32)
    activated = gelu_exact(hidden_f).astype(jnp.bfloat16)
    back_hidden = jnp.dot(upstream, w_out.T, preferred_element_type=jnp.float32)
    grad_hidden = jax.vjp(gelu_exact, hidden_f)[1](back_hidden)[0].astype(jnp.bfloat16)
    total_out = total_out + jnp.dot(activated.T, upstream, preferred_element_type=jnp.float32)
    total_in = total_in + jnp.dot(mixed.T, grad_hidden, preferred_element_type=jnp.float32)
    total_bias = total_bias + lax.optimization_barrier(jnp.sum(grad_hidden.astype(jnp.float32), axis=0))
    block = FF // N_TP
    hidden_blocks = grad_hidden.reshape(length, N_TP, block).astype(jnp.float32)
    weight_blocks = w_in.reshape(D, N_TP, block).astype(jnp.float32)
    parts = jnp.einsum('lnf,dnf->nld', hidden_blocks, weight_blocks).astype(jnp.bfloat16)
    parts = lax.optimization_barrier(parts).astype(jnp.float32)
    grad_mixed = (upstream.astype(jnp.float32) + lax.optimization_barrier(jnp.sum(parts, axis=0))).astype(jnp.bfloat16)
    grad_f = grad_mixed.astype(jnp.float32)
    grad_pad = jnp.pad(grad_f, ((3, 3), (0, 0)))
    grad_inputs = grad_f
    taps = []
    for tap in range(KW):
        grad_inputs = grad_inputs + kernel[tap] * grad_pad[6 - tap:6 - tap + length]
        taps.append(lax.optimization_barrier(jnp.sum(grad_f * padded[tap:tap + length], axis=0)))
    total_kernel = total_kernel + jnp.stack(taps)
    return ((total_in, total_out, total_bias, total_kernel), grad_inputs.astype(jnp.bfloat16))

def reference(inputs, saved_hidden, upstream, w_in, w_out, kernel):
    start = (jnp.zeros((D, FF), jnp.float32), jnp.zeros((FF, D), jnp.float32), jnp.zeros((FF,), jnp.float32), jnp.zeros((KW, D), jnp.float32))
    step = partial(one_sequence, w_in=w_in, w_out=w_out, kernel=kernel)
    totals, grad_inputs = lax.scan(step, start, (inputs, saved_hidden, upstream))
    return (grad_inputs, totals[0], totals[1], totals[2], totals[3])
```

```python
import functools

import jax
import jax.numpy as jnp
from jax import lax
from jax.experimental import pallas as pl
from jax.experimental.pallas import tpu as pltpu
from jax.sharding import PartitionSpec as P

KW = 7
D = 1280
H = 320
T = 192
SLOTS = 16
HR = 48
SR = 2 * HR
HOPS = SLOTS - 2
HALO = 16
MESH_ID = pl.DeviceIdType.MESH
F32 = jnp.float32
BF16 = jnp.bfloat16

LAG = 8
MIXED_AT = 4
GWO_AT = ((16, 17), (24, 25))
GWI_AT = ((22, 23), (30, 31))
DX_FROM = 26
RED_AT = ((26, 28, 33, 36, 39), (32, 34, 39, None, None))
STEPS = 3 * HOPS + 2


def dot_nt(a, b):
    return lax.dot_general(a, b, (((1,), (1,)), ((), ())), preferred_element_type=F32)


def gelu_parts(x):
    a = jnp.abs(x) * 0.7071067811865476
    t = 1.0 / (1.0 + 0.5 * a)
    p = 0.17087277
    for coef in (
        -0.82215223,
        1.48851587,
        -1.13520398,
        0.27886807,
        -0.18628806,
        0.09678418,
        0.37409196,
        1.00002368,
        -1.26551223,
    ):
        p = p * t + coef
    square = a * a
    tail = 0.5 * t * jnp.exp(p - square)
    cdf = jnp.where(x >= 0, 1.0 - tail, tail)
    slope = cdf + x * (0.3989422804014327 * jnp.exp(-square))
    return x * cdf, slope


def body(
    x_hbm, h_hbm, u_hbm, wi_hbm, wo_hbm, k_ref,
    gi_hbm, gwo_hbm, gwi_hbm, sm_ref,
    up, mx, dx, rr, hh, act, gh, wo, wi, gwo, gwi, actt, bias,
    cs, cr, ys, yr, xs, xr, fout,
    xb, xf, gf, gmb, gio, gib, sm, smc, smy, smx, smz, smf,
    z_send, z_recv, h_send, h_recv, h_load, w_send, w_recv, l_sem, o_sem,
    halo_send, halo_recv, red_send, red_recv, s_send, s_recv,
):
    dp, tp = lax.axis_index("dp"), lax.axis_index("tp")
    xl, y, c = dp // 8, (dp // 2) % 4, dp % 2
    z, xh = tp // 2, tp % 2
    me_x = xh * 2 + xl

    def z_dev(n):
        return (dp, (tp + 2 * n + 32) % 16)

    def y_dev(n):
        return (xl * 8 + ((y + n) % 4) * 2 + c, tp)

    core_dev = (dp + 1 - 2 * c, tp)
    xh_dev = (dp, tp + 1 - 2 * xh)
    xl_dev = (dp + 8 - 16 * xl, tp)
    xd_dev = (dp + 8 - 16 * xl, tp + 1 - 2 * xh)
    next_dev = (dp, (tp + 1) % 16)
    prev_dev = (dp, (tp + 15) % 16)

    def remote(src, dst, send, recv, device):
        return pltpu.make_async_remote_copy(
            src_ref=src, dst_ref=dst, send_sem=send, recv_sem=recv,
            device_id=device, device_id_type=MESH_ID,
        )

    def local_loads():
        copies = []
        n = 0
        for a in range(2):
            for half in range(2):
                copies.append(pltpu.make_async_copy(
                    u_hbm.at[0, pl.ds(half * 96 + a * HR, HR)], up.at[a, pl.ds(half * HR, HR)], l_sem.at[n]))
                n += 1
        copies.append(pltpu.make_async_copy(x_hbm.at[0], xb.at[pl.ds(HALO, T)], l_sem.at[n]))
        copies.append(pltpu.make_async_copy(wo_hbm, wo.at[0], l_sem.at[n + 1]))
        copies.append(pltpu.make_async_copy(wi_hbm, wi.at[0], l_sem.at[n + 2]))
        return copies

    def hidden_rows(slot, half, parity):
        s, a = slot // 2, slot % 2
        block = 2 * ((z + (s if half else 8 - s)) % 8) + parity
        start = pl.multiple_of(block * T + half * 96 + a * HR, 16)
        return h_hbm.at[0, pl.ds(start, HR)]

    def hidden_load(slot, half):
        return pltpu.make_async_copy(
            hidden_rows(slot, half, xh), hh.at[0, slot, pl.ds(half * HR, HR)], h_load.at[slot, half])

    def hidden_send(slot, half):
        return remote(
            hidden_rows(slot, half, 1 - xh), hh.at[1, slot, pl.ds(half * HR, HR)],
            h_send.at[slot, half], h_recv.at[slot, half], xh_dev)

    wo_copy = remote(wo_hbm, wo.at[1], w_send.at[0], w_recv.at[0], xh_dev)
    wi_copy = remote(wi_hbm, wi.at[1], w_send.at[1], w_recv.at[1], xh_dev)
    halo_copies = (
        remote(x_hbm.at[0, pl.ds(T - HALO, HALO)], xb.at[pl.ds(0, HALO)], halo_send.at[0], halo_recv.at[0], next_dev),
        remote(x_hbm.at[0, pl.ds(0, HALO)], xb.at[pl.ds(T + HALO, HALO)], halo_send.at[1], halo_recv.at[1], prev_dev),
    )

    def ring(phase, hop, half):
        rows = pl.ds(half * HR, HR)
        device = z_dev(-1 if half else 1)
        if phase == 0:
            src, dst = up.at[hop, rows], up.at[hop + 2, rows]
        elif phase == 1:
            src, dst = mx.at[hop, rows], mx.at[hop + 2, rows]
        else:
            src, dst = dx.at[hop + 2, rows], rr.at[hop, rows]
        return remote(src, dst, z_send.at[phase, hop, half], z_recv.at[phase, hop, half], device)

    locals_ = local_loads()
    for copy in locals_:
        copy.start()
    barrier = pltpu.get_barrier_semaphore()
    peers = [z_dev(n) for n in range(1, 8)] + [y_dev(n) for n in range(1, 4)]
    peers += [core_dev, xl_dev, xd_dev, next_dev, prev_dev]
    for peer in peers:
        pl.semaphore_signal(barrier, inc=1, device_id=peer, device_id_type=MESH_ID)
    pl.semaphore_wait(barrier, len(peers))

    for copy in halo_copies:
        copy.start()
    wo_copy.start()

    @pl.loop(0, SLOTS)
    def _(slot):
        for half in range(2):
            hidden_load(slot, half).start()

    bias[...] = jnp.zeros_like(bias)

    def red_core(m):
        return remote(cs.at[m, 1 - c], cr.at[m], red_send.at[m, 0], red_recv.at[m, 0], core_dev)

    def red_y(m, n):
        return remote(ys.at[m, (y + n) % 4], yr.at[m, n - 1], red_send.at[m, n], red_recv.at[m, n], y_dev(n))

    def red_x(m):
        return (
            remote(xs.at[m, 0], xr.at[m, me_x], red_send.at[m, 4], red_recv.at[m, 4], xl_dev),
            remote(xs.at[m, 1], xr.at[m, me_x], red_send.at[m, 5], red_recv.at[m, 5], xh_dev),
            remote(xs.at[m, 1], xr.at[m, me_x], red_send.at[m, 6], red_recv.at[m, 6], xd_dev),
        )

    def red_x_wait(m):
        for sem, src_x, device in (
            (4, xh * 2 + 1 - xl, xl_dev), (5, (1 - xh) * 2 + xl, xh_dev), (6, (1 - xh) * 2 + 1 - xl, xd_dev),
        ):
            remote(xs.at[m, 0], xr.at[m, src_x], red_send.at[m, sem], red_recv.at[m, sem], device).wait_recv()

    def ag_y(m, n, source):
        return remote(
            fout.at[m, c, source], fout.at[m, c, source], red_send.at[m, 6 + n], red_recv.at[m, 6 + n], y_dev(n))

    def ag_core(m, half):
        return remote(fout.at[m, half], fout.at[m, half], red_send.at[m, 10], red_recv.at[m, 10], core_dev)

    totals = (gwo, gwi)

    def reduce_stage(m, stage):
        total = totals[m]
        if stage == 0:
            for q in range(2):
                for half in range(2):
                    cs[m, half, q] = total[q, :, half * 640:(half + 1) * 640].astype(BF16)
            red_core(m).start()
        elif stage == 1:
            red_core(m).wait_recv()
            own_cols = pl.ds(pl.multiple_of(c * 640, 128), 640)
            for q in range(2):
                for part in range(4):
                    rows = slice(part * 80, part * 80 + 80)
                    ys[m, part, q] = (total[q, rows, own_cols] + cr[m, q, rows].astype(F32)).astype(BF16)
            for n in range(1, 4):
                red_y(m, n).start()
        elif stage == 2:
            for n in range(1, 4):
                red_y(m, n).wait_recv()
            for q in range(2):
                part = ys[m, y, q].astype(F32)
                for n in range(3):
                    part = part + yr[m, n, q].astype(F32)
                xs[m, q] = part.astype(BF16)
            for copy in red_x(m):
                copy.start()
        elif stage == 3:
            red_x_wait(m)
            xr[m, me_x] = xs[m, 0]
            part = xr[m, 0].astype(F32)
            for n in range(1, 4):
                part = part + xr[m, n].astype(F32)
            fout[m, c, y] = part.astype(BF16)
            for n in range(1, 4):
                ag_y(m, n, y).start()
        else:
            for n in range(1, 4):
                ag_y(m, n, (y + 4 - n) % 4).wait_recv()
            ag_core(m, c).start()

    def reduce_out(m):
        return pltpu.make_async_copy(fout.at[m], (gwo_hbm, gwi_hbm)[m], o_sem.at[m])

    def mixed_task():
        locals_[4].wait()
        for copy in halo_copies:
            copy.wait_recv()
        xf[pl.ds(HALO, T)] = xb[pl.ds(HALO, T)].astype(F32)
        xf[pl.ds(0, HALO)] = jnp.where(tp == 0, 0.0, xb[pl.ds(0, HALO)].astype(F32))
        xf[pl.ds(T + HALO, HALO)] = jnp.where(tp == 15, 0.0, xb[pl.ds(T + HALO, HALO)].astype(F32))

        @pl.loop(0, D // 128)
        def _(n):
            cols = pl.ds(pl.multiple_of(n * 128, 128), 128)
            taps = k_ref[:, cols]
            out = xf[HALO:HALO + T, cols]
            for tap in range(KW):
                out = out + taps[tap:tap + 1] * xf[HALO - 3 + tap:HALO - 3 + tap + T, cols]
            out = out.astype(BF16)
            for a in range(2):
                for half in range(2):
                    start = half * 96 + a * HR
                    mx[a, half * HR:(half + 1) * HR, cols] = out[start:start + HR]

    def hidden_task(slot):
        for half in range(2):
            hidden_load(slot, half).wait()
            hidden_send(slot, half).wait_recv()
        rows = up[slot]
        for q in range(2):
            back = dot_nt(rows, wo[q])
            value, slope = gelu_parts(hh[q, slot].astype(F32))
            grad = (slope * back).astype(BF16)
            act[q, slot] = value.astype(BF16)
            gh[q, slot] = grad
            bias[q] += jnp.sum(grad.astype(F32).reshape(SR // 8, 8, H), axis=0)

    def weight_task(left, right, total, q, part):
        eight = pl.ds(part * 8, 8)
        actt[...] = left[q, eight].reshape(8 * SR, H).T

        @pl.loop(0, D // 256)
        def _(n):
            cols = pl.ds(pl.multiple_of(n * 256, 256), 256)
            value = jnp.dot(
                actt[...], right[eight, :, cols].reshape(8 * SR, 256), preferred_element_type=F32)
            if part == 0:
                total[q, :, cols] = value
            else:
                total[q, :, cols] += value

    def dx_task(slot):
        g0, g1 = gh[0, slot], gh[1, slot]
        for n in range(D // 256):
            rows = slice(n * 256, n * 256 + 256)
            dx[slot, :, rows] = (dot_nt(g0, wi[0, rows]) + dot_nt(g1, wi[1, rows])).astype(BF16)

    for n in range(4):
        locals_[n].wait()

    def at(step, i):
        return pl.when(i == step)

    def step(i, carry):
        @pl.when((i >= 2) & (i < 16))
        def _():
            for half in range(2):
                ring(0, i - 2, half).wait_recv()

        @pl.when(i < HOPS)
        def _():
            for half in range(2):
                ring(0, i, half).start()

        @pl.when((i >= 16) & (i < 30))
        def _():
            for half in range(2):
                ring(1, i - 16, half).wait_recv()

        @pl.when((i >= 14) & (i < 28))
        def _():
            for half in range(2):
                ring(1, i - 14, half).start()

        @pl.when((i >= 30) & (i < 42))
        def _():
            for half in range(2):
                ring(2, i - 30, half).wait_recv()
            slot = i - 26
            dx[slot] = (dx[slot].astype(F32) + rr[i - 30].astype(F32)).astype(BF16)

        @pl.when((i >= 28) & (i < 42))
        def _():
            for half in range(2):
                ring(2, i - 28, half).start()

        @pl.when(i < 8)
        def _():
            for j in range(2):
                for half in range(2):
                    hidden_send(2 * i + j, half).start()

        @at(8, i)
        def _():
            wi_copy.start()
            locals_[5].wait()
            wo_copy.wait_recv()

        at(MIXED_AT, i)(mixed_task)

        @pl.when((i >= LAG) & (i < LAG + SLOTS))
        def _():
            hidden_task(i - LAG)

        for part in range(2):
            for q in range(2):
                at(GWO_AT[part][q], i)(functools.partial(weight_task, act, up, gwo, q, part))
                at(GWI_AT[part][q], i)(functools.partial(weight_task, gh, mx, gwi, q, part))

        @at(DX_FROM, i)
        def _():
            locals_[6].wait()
            wi_copy.wait_recv()

        @pl.when((i >= DX_FROM) & (i < DX_FROM + SLOTS))
        def _():
            dx_task((i - DX_FROM + 2) % SLOTS)

        for m in range(2):
            for stage in range(5):
                if RED_AT[m][stage] is not None:
                    at(RED_AT[m][stage], i)(functools.partial(reduce_stage, m, stage))
        return carry

    lax.fori_loop(0, STEPS - 2, step, 0)

    for a in range(2):
        for half in range(2):
            ring(2, HOPS - 2 + a, half).wait_recv()
        done = up[a].astype(F32) + (dx[a].astype(F32) + rr[HOPS - 2 + a].astype(F32))
        done = done.astype(BF16)
        for half in range(2):
            start = half * 96 + a * HR
            gmb[start:start + HR] = done[half * HR:(half + 1) * HR]
            gf[HALO + start:HALO + start + HR] = done[half * HR:(half + 1) * HR].astype(F32)
    edge_copies = (
        remote(gmb.at[pl.ds(T - HALO, HALO)], gib.at[0], halo_send.at[2], halo_recv.at[2], next_dev),
        remote(gmb.at[pl.ds(0, HALO)], gib.at[1], halo_send.at[3], halo_recv.at[3], prev_dev),
    )
    for copy in edge_copies:
        copy.start()

    reduce_stage(1, 3)

    sm[7:8] = jnp.zeros((1, D), F32)
    b0 = jnp.sum(bias[0], axis=0, keepdims=True)
    b1 = jnp.sum(bias[1], axis=0, keepdims=True)
    sm[7:8, 0:H] = jnp.where(xh == 0, b0, b1)
    sm[7:8, 384:384 + H] = jnp.where(xh == 0, b1, b0)

    @pl.loop(0, D // 128)
    def _(n):
        cols = pl.ds(pl.multiple_of(n * 128, 128), 128)
        grad = gf[HALO:HALO + T, cols]
        for tap in range(KW):
            product = grad * xf[HALO - 3 + tap:HALO - 3 + tap + T, cols]
            sm[tap:tap + 1, cols] = jnp.sum(product, axis=0, keepdims=True)

    def sm_core():
        return remote(sm, smc, s_send.at[0], s_recv.at[0], core_dev)

    def sm_y(n, source):
        return remote(smy.at[source], smy.at[source], s_send.at[n], s_recv.at[n], y_dev(n))

    def sm_x(n, source, device):
        return remote(smx.at[source], smx.at[source], s_send.at[4 + n], s_recv.at[4 + n], device)

    def sm_z(n, source):
        return remote(smz.at[source], smz.at[source], s_send.at[6 + n], s_recv.at[6 + n], z_dev(n))

    def sm_last(half):
        return remote(smf.at[half], smf.at[half], s_send.at[14], s_recv.at[14], core_dev)

    sm_core().start()

    reduce_stage(1, 4)

    sm_core().wait_recv()
    own_cols = pl.ds(pl.multiple_of(c * 640, 128), 640)
    smy[y] = sm[:, own_cols] + smc[:, own_cols]
    for n in range(1, 4):
        sm_y(n, y).start()

    for copy in edge_copies:
        copy.wait_recv()
    gf[pl.ds(0, HALO)] = jnp.where(tp == 0, 0.0, gib[0].astype(F32))
    gf[pl.ds(T + HALO, HALO)] = jnp.where(tp == 15, 0.0, gib[1].astype(F32))

    for n in range(1, 4):
        sm_y(n, (y + 4 - n) % 4).wait_recv()
    smx[me_x] = (smy[0] + smy[1]) + (smy[2] + smy[3])
    x_devices = (xl_dev, xh_dev, xd_dev)
    for n in range(3):
        sm_x(n, me_x, x_devices[n]).start()

    @pl.loop(0, D // 128)
    def _(n):
        cols = pl.ds(pl.multiple_of(n * 128, 128), 128)
        taps = k_ref[:, cols]
        out = gf[HALO:HALO + T, cols]
        for tap in range(KW):
            out = out + taps[tap:tap + 1] * gf[HALO + 3 - tap:HALO + 3 - tap + T, cols]
        gio[:, cols] = out.astype(BF16)

    gi_out = pltpu.make_async_copy(gio, gi_hbm.at[0], o_sem.at[2])
    gi_out.start()

    for n, source in enumerate((xh * 2 + 1 - xl, (1 - xh) * 2 + xl, (1 - xh) * 2 + 1 - xl)):
        sm_x(n, source, x_devices[n]).wait_recv()
    summed = (smx[0] + smx[1]) + (smx[2] + smx[3])
    smz[z] = summed
    for n in range(1, 8):
        sm_z(n, z).start()

    ag_core(1, 1 - c).wait_recv()
    ag_core(0, 1 - c).wait_recv()
    for m in range(2):
        reduce_out(m).start()

    for n in range(1, 8):
        sm_z(n, (z + 8 - n) % 8).wait_recv()
    whole = smz[0]
    for n in range(1, 8):
        whole = whole + smz[n]
    row = lax.broadcasted_iota(jnp.int32, (8, 640), 0)
    smf[c] = jnp.where(row == 7, smz[z], whole)
    sm_last(c).start()

    @pl.loop(0, HOPS)
    def _(hop):
        for phase in range(3):
            for half in range(2):
                ring(phase, hop, half).wait_send()

    @pl.loop(0, SLOTS)
    def _(slot):
        for half in range(2):
            hidden_send(slot, half).wait_send()

    wo_copy.wait_send()
    wi_copy.wait_send()
    for copy in halo_copies + edge_copies:
        copy.wait_send()
    for m in range(2):
        red_core(m).wait_send()
        for n in range(1, 4):
            red_y(m, n).wait_send()
            ag_y(m, n, y).wait_send()
        for copy in red_x(m):
            copy.wait_send()
        ag_core(m, c).wait_send()
    sm_core().wait_send()
    for n in range(1, 4):
        sm_y(n, y).wait_send()
    for n in range(3):
        sm_x(n, me_x, x_devices[n]).wait_send()
    for n in range(1, 8):
        sm_z(n, z).wait_send()
    gi_out.wait()
    for m in range(2):
        reduce_out(m).wait()
    sm_last(1 - c).wait_recv()
    sm_ref[...] = smf[...]
    sm_last(c).wait_send()


def shards(inputs, saved_hidden, upstream, w_in, w_out, kernel):
    anyspace = pl.BlockSpec(memory_space=pl.ANY)
    vmem = pl.BlockSpec(memory_space=pltpu.VMEM)
    dma = pltpu.SemaphoreType.DMA
    grad_inputs, gwo, gwi, small = pl.pallas_call(
        body,
        out_shape=(
            jax.ShapeDtypeStruct((1, T, D), BF16),
            jax.ShapeDtypeStruct((2, 4, 80, 640), BF16),
            jax.ShapeDtypeStruct((2, 4, 80, 640), BF16),
            jax.ShapeDtypeStruct((2, 8, 640), F32),
        ),
        in_specs=[anyspace] * 5 + [vmem],
        out_specs=(anyspace, anyspace, anyspace, vmem),
        scratch_shapes=[
            pltpu.VMEM((SLOTS, SR, D), BF16),
            pltpu.VMEM((SLOTS, SR, D), BF16),
            pltpu.VMEM((SLOTS, SR, D), BF16),
            pltpu.VMEM((HOPS, SR, D), BF16),
            pltpu.VMEM((2, SLOTS, SR, H), BF16),
            pltpu.VMEM((2, SLOTS, SR, H), BF16),
            pltpu.VMEM((2, SLOTS, SR, H), BF16),
            pltpu.VMEM((2, H, D), BF16),
            pltpu.VMEM((2, D, H), BF16),
            pltpu.VMEM((2, H, D), F32),
            pltpu.VMEM((2, H, D), F32),
            pltpu.VMEM((H, 8 * SR), BF16),
            pltpu.VMEM((2, 8, H), F32),
            pltpu.VMEM((2, 2, 2, H, 640), BF16),
            pltpu.VMEM((2, 2, H, 640), BF16),
            pltpu.VMEM((2, 4, 2, 80, 640), BF16),
            pltpu.VMEM((2, 3, 2, 80, 640), BF16),
            pltpu.VMEM((2, 2, 80, 640), BF16),
            pltpu.VMEM((2, 4, 80, 640), BF16),
            pltpu.VMEM((2, 2, 4, 80, 640), BF16),
            pltpu.VMEM((T + 2 * HALO, D), BF16),
            pltpu.VMEM((T + 2 * HALO, D), F32),
            pltpu.VMEM((T + 2 * HALO, D), F32),
            pltpu.VMEM((T, D), BF16),
            pltpu.VMEM((T, D), BF16),
            pltpu.VMEM((2, HALO, D), BF16),
            pltpu.VMEM((8, D), F32),
            pltpu.VMEM((8, D), F32),
            pltpu.VMEM((4, 8, 640), F32),
            pltpu.VMEM((4, 8, 640), F32),
            pltpu.VMEM((8, 8, 640), F32),
            pltpu.VMEM((2, 8, 640), F32),
            dma((3, HOPS, 2)), dma((3, HOPS, 2)),
            dma((SLOTS, 2)), dma((SLOTS, 2)), dma((SLOTS, 2)),
            dma((2,)), dma((2,)), dma((7,)), dma((3,)),
            dma((4,)), dma((4,)),
            dma((2, 11)), dma((2, 11)),
            dma((15,)), dma((15,)),
        ],
        compiler_params=pltpu.CompilerParams(
            collective_id=0, has_side_effects=True, vmem_limit_bytes=64 * 1024 * 1024 - 65536),
        name="step",
    )(inputs, saved_hidden, upstream, w_in, w_out, kernel)
    grad_w_out = jnp.concatenate([gwo[0].reshape(H, 640), gwo[1].reshape(H, 640)], axis=1).astype(F32)
    grad_w_in = gwi.reshape(2, H, 640).transpose(0, 2, 1).reshape(D, H).astype(F32)
    small = jnp.concatenate([small[0], small[1]], axis=1)
    parity = lax.axis_index("tp") % 2
    grad_bias = jnp.where(parity == 0, small[7, :H], small[7, 384:384 + H])
    return grad_inputs, grad_w_in, grad_w_out, grad_bias, small[:KW]


def solution(mesh):
    in_specs = (
        P("dp", "tp", None), P("dp", None, "tp"), P("dp", "tp", None), P(None, "tp"), P("tp", None), P())
    out_specs = (P("dp", "tp", None), P(None, "tp"), P("tp", None), P("tp"), P())
    return jax.shard_map(shards, mesh=mesh, in_specs=in_specs, out_specs=out_specs, check_vma=False)
```

```python
import functools

import jax
import jax.numpy as jnp
from jax import lax
from jax.experimental import pallas as pl
from jax.experimental.pallas import tpu as pltpu
from jax.sharding import PartitionSpec as P

KW = 7
D = 1280
H = 320
T = 192
SLOTS = 16
HR = 48
SR = 2 * HR
HOPS = SLOTS - 2
HALO = 16
MESH_ID = pl.DeviceIdType.MESH
F32 = jnp.float32
BF16 = jnp.bfloat16

LAG = 8
MIXED_AT = 4
GWO_AT = ((16, 17), (24, 25))
GWI_AT = ((22, 23), (30, 31))
DX_FROM = 26
RED_AT = ((26, 28, 33, 36, 39), (31, 32, 36, 39, None))
STEPS = 3 * HOPS + 2


def dot_nt(a, b):
    return lax.dot_general(a, b, (((1,), (1,)), ((), ())), preferred_element_type=F32)


def gelu_parts(x):
    a = jnp.abs(x) * 0.7071067811865476
    t = 1.0 / (1.0 + 0.5 * a)
    p = 0.17087277
    for coef in (
        -0.82215223,
        1.48851587,
        -1.13520398,
        0.27886807,
        -0.18628806,
        0.09678418,
        0.37409196,
        1.00002368,
        -1.26551223,
    ):
        p = p * t + coef
    square = a * a
    tail = 0.5 * t * jnp.exp(p - square)
    cdf = jnp.where(x >= 0, 1.0 - tail, tail)
    slope = cdf + x * (0.3989422804014327 * jnp.exp(-square))
    return x * cdf, slope


def body(
    x_hbm, h_hbm, u_hbm, wi_hbm, wo_hbm, k_ref,
    gi_hbm, gwo_hbm, gwi_hbm, sm_ref,
    up, mx, dx, rr, ht, hrow, hh, act, gh, wo, wi, gwo, gwi, actt, bias,
    cs, cr, ys, yr, xs, xr, fout,
    xb, xf, gf, gmb, gio, gib, sm, sms, smc, smy, smx, smz,
    z_send, z_recv, h_send, h_recv, h_load, w_send, w_recv, l_sem, o_sem,
    halo_send, halo_recv, red_send, red_recv, s_send, s_recv,
):
    dp, tp = lax.axis_index("dp"), lax.axis_index("tp")
    xl, y, c = dp // 8, (dp // 2) % 4, dp % 2
    z, xh = tp // 2, tp % 2
    me_x = xh * 2 + xl

    def z_dev(n):
        return (dp, (tp + 2 * n + 32) % 16)

    def y_dev(n):
        return (xl * 8 + ((y + n) % 4) * 2 + c, tp)

    core_dev = (dp + 1 - 2 * c, tp)
    xh_dev = (dp, tp + 1 - 2 * xh)
    xl_dev = (dp + 8 - 16 * xl, tp)
    xd_dev = (dp + 8 - 16 * xl, tp + 1 - 2 * xh)
    next_dev = (dp, (tp + 1) % 16)
    prev_dev = (dp, (tp + 15) % 16)

    def remote(src, dst, send, recv, device):
        return pltpu.make_async_remote_copy(
            src_ref=src, dst_ref=dst, send_sem=send, recv_sem=recv,
            device_id=device, device_id_type=MESH_ID,
        )

    def local_loads():
        copies = []
        n = 0
        for a in range(2):
            for half in range(2):
                copies.append(pltpu.make_async_copy(
                    u_hbm.at[0, pl.ds(half * 96 + a * HR, HR)], up.at[a, pl.ds(half * HR, HR)], l_sem.at[n]))
                n += 1
        copies.append(pltpu.make_async_copy(x_hbm.at[0], xb.at[pl.ds(HALO, T)], l_sem.at[n]))
        copies.append(pltpu.make_async_copy(wo_hbm, wo.at[0], l_sem.at[n + 1]))
        copies.append(pltpu.make_async_copy(wi_hbm, wi.at[0], l_sem.at[n + 2]))
        return copies

    def hidden_chunk(n):
        return (z + 8 + ((n + 1) // 2) * (1 - 2 * (n % 2))) % 8

    def hidden_load(n):
        chunk = hidden_chunk(n)
        cols = pl.ds(pl.multiple_of(chunk * 2 * T, 128), 2 * T)
        return pltpu.make_async_copy(h_hbm.at[0, :, cols], ht.at[chunk], h_load.at[n])

    def hidden_rows(slot, half, parity):
        s, a = slot // 2, slot % 2
        chunk = (z + (s if half else 8 - s)) % 8
        return chunk, pl.ds(pl.multiple_of(parity * T + half * 96 + a * HR, 16), HR)

    def hidden_send(slot, half):
        chunk, rows = hidden_rows(slot, half, 1 - xh)
        return remote(
            hrow.at[chunk, rows], hh.at[slot, pl.ds(half * HR, HR)],
            h_send.at[slot, half], h_recv.at[slot, half], xh_dev)

    wo_copy = remote(wo_hbm, wo.at[1], w_send.at[0], w_recv.at[0], xh_dev)
    wi_copy = remote(wi_hbm, wi.at[1], w_send.at[1], w_recv.at[1], xh_dev)
    halo_copies = (
        remote(x_hbm.at[0, pl.ds(T - HALO, HALO)], xb.at[pl.ds(0, HALO)], halo_send.at[0], halo_recv.at[0], next_dev),
        remote(x_hbm.at[0, pl.ds(0, HALO)], xb.at[pl.ds(T + HALO, HALO)], halo_send.at[1], halo_recv.at[1], prev_dev),
    )

    def ring(phase, hop, half):
        rows = pl.ds(half * HR, HR)
        device = z_dev(-1 if half else 1)
        if phase == 0:
            src, dst = up.at[hop, rows], up.at[hop + 2, rows]
        elif phase == 1:
            src, dst = mx.at[hop, rows], mx.at[hop + 2, rows]
        else:
            src, dst = dx.at[hop + 2, rows], rr.at[hop, rows]
        return remote(src, dst, z_send.at[phase, hop, half], z_recv.at[phase, hop, half], device)

    locals_ = local_loads()
    for copy in locals_:
        copy.start()
    for n in range(8):
        hidden_load(n).start()
    barrier = pltpu.get_barrier_semaphore()
    peers = [z_dev(1), z_dev(-1)] + [y_dev(n) for n in range(1, 4)]
    peers += [core_dev, xl_dev, xh_dev, xd_dev, next_dev, prev_dev]
    for peer in peers:
        pl.semaphore_signal(barrier, inc=1, device_id=peer, device_id_type=MESH_ID)
    pl.semaphore_wait(barrier, len(peers))

    for copy in halo_copies:
        copy.start()
    wo_copy.start()

    bias[...] = jnp.zeros_like(bias)

    def red_core(m):
        return remote(cs.at[m, 1 - c], cr.at[m], red_send.at[m, 0], red_recv.at[m, 0], core_dev)

    def red_y(m, n):
        return remote(ys.at[m, (y + n) % 4], yr.at[m, n - 1], red_send.at[m, n], red_recv.at[m, n], y_dev(n))

    def red_x(m):
        return (
            remote(xs.at[m, 0], xr.at[m, me_x], red_send.at[m, 4], red_recv.at[m, 4], xl_dev),
            remote(xs.at[m, 1], xr.at[m, me_x], red_send.at[m, 5], red_recv.at[m, 5], xh_dev),
            remote(xs.at[m, 1], xr.at[m, me_x], red_send.at[m, 6], red_recv.at[m, 6], xd_dev),
        )

    def red_x_wait(m):
        for sem, src_x, device in (
            (4, xh * 2 + 1 - xl, xl_dev), (5, (1 - xh) * 2 + xl, xh_dev), (6, (1 - xh) * 2 + 1 - xl, xd_dev),
        ):
            remote(xs.at[m, 0], xr.at[m, src_x], red_send.at[m, sem], red_recv.at[m, sem], device).wait_recv()

    def ag_y(m, n, source):
        return remote(
            fout.at[m, c, pl.ds(source * 80, 80)], fout.at[m, c, pl.ds(source * 80, 80)], red_send.at[m, 6 + n], red_recv.at[m, 6 + n], y_dev(n))

    def ag_core(m, half):
        return remote(fout.at[m, half], fout.at[m, half], red_send.at[m, 10], red_recv.at[m, 10], core_dev)

    totals = (gwo, gwi)

    def reduce_stage(m, stage):
        total = totals[m]
        if stage == 0:
            for q in range(2):
                for half in range(2):
                    cs[m, half, q] = total[q, :, half * 640:(half + 1) * 640].astype(BF16)
            red_core(m).start()
        elif stage == 1:
            red_core(m).wait_recv()
            own_cols = pl.ds(pl.multiple_of(c * 640, 128), 640)
            for q in range(2):
                for part in range(4):
                    rows = slice(part * 80, part * 80 + 80)
                    ys[m, part, q] = (total[q, rows, own_cols] + cr[m, q, rows].astype(F32)).astype(BF16)
            for n in range(1, 4):
                red_y(m, n).start()
        elif stage == 2:
            for n in range(1, 4):
                red_y(m, n).wait_recv()
            for q in range(2):
                part = ys[m, y, q].astype(F32)
                for n in range(3):
                    part = part + yr[m, n, q].astype(F32)
                xs[m, q] = part.astype(BF16)
            for copy in red_x(m):
                copy.start()
        elif stage == 3:
            red_x_wait(m)
            xr[m, me_x] = xs[m, 0]
            part = xr[m, 0].astype(F32)
            for n in range(1, 4):
                part = part + xr[m, n].astype(F32)
            fout[m, c, pl.ds(y * 80, 80)] = part.astype(BF16)
            for n in range(1, 4):
                ag_y(m, n, y).start()
        else:
            for n in range(1, 4):
                ag_y(m, n, (y + 4 - n) % 4).wait_recv()
            ag_core(m, c).start()

    def reduce_out(m, half):
        cols = pl.ds(half * 640, 640)
        return pltpu.make_async_copy(fout.at[m, half], (gwo_hbm, gwi_hbm)[m].at[:, cols], o_sem.at[m, half])

    def mixed_task():
        locals_[4].wait()
        for copy in halo_copies:
            copy.wait_recv()
        xf[pl.ds(HALO, T)] = xb[pl.ds(HALO, T)].astype(F32)
        xf[pl.ds(0, HALO)] = jnp.where(tp == 0, 0.0, xb[pl.ds(0, HALO)].astype(F32))
        xf[pl.ds(T + HALO, HALO)] = jnp.where(tp == 15, 0.0, xb[pl.ds(T + HALO, HALO)].astype(F32))

        @pl.loop(0, D // 128)
        def _(n):
            cols = pl.ds(pl.multiple_of(n * 128, 128), 128)
            taps = k_ref[:, cols]
            out = xf[HALO:HALO + T, cols]
            for tap in range(KW):
                out = out + taps[tap:tap + 1] * xf[HALO - 3 + tap:HALO - 3 + tap + T, cols]
            out = out.astype(BF16)
            for a in range(2):
                for half in range(2):
                    start = half * 96 + a * HR
                    mx[a, half * HR:(half + 1) * HR, cols] = out[start:start + HR]

    def hidden_task(slot):
        for half in range(2):
            hidden_send(slot, half).wait_recv()
        rows = up[slot]
        own = []
        for half in range(2):
            chunk, where = hidden_rows(slot, half, xh)
            own.append(hrow[chunk, where])
        own = jnp.concatenate(own, axis=0)
        for q in range(2):
            back = dot_nt(rows, wo[q])
            value, slope = gelu_parts((hh[slot] if q else own).astype(F32))
            grad = (slope * back).astype(BF16)
            act[q, slot] = value.astype(BF16)
            gh[q, slot] = grad
            bias[q] += jnp.sum(grad.astype(F32).reshape(SR // 8, 8, H), axis=0)

    def weight_task(left, right, total, q, part):
        eight = pl.ds(part * 8, 8)
        actt[...] = left[q, eight].reshape(8 * SR, H).T

        @pl.loop(0, D // 256)
        def _(n):
            cols = pl.ds(pl.multiple_of(n * 256, 256), 256)
            value = jnp.dot(
                actt[...], right[eight, :, cols].reshape(8 * SR, 256), preferred_element_type=F32)
            if part == 0:
                total[q, :, cols] = value
            else:
                total[q, :, cols] += value

    def dx_task(slot):
        g0, g1 = gh[0, slot], gh[1, slot]
        for n in range(D // 256):
            rows = slice(n * 256, n * 256 + 256)
            dx[slot, :, rows] = (
                jnp.dot(g0, wi[0, :, rows], preferred_element_type=F32)
                + jnp.dot(g1, wi[1, :, rows], preferred_element_type=F32)
            ).astype(BF16)

    for n in range(4):
        locals_[n].wait()

    def at(step, i):
        return pl.when(i == step)

    def step(i, carry):
        @pl.when((i >= 2) & (i < 16))
        def _():
            for half in range(2):
                ring(0, i - 2, half).wait_recv()

        @pl.when(i < HOPS)
        def _():
            for half in range(2):
                ring(0, i, half).start()

        @pl.when((i >= 16) & (i < 30))
        def _():
            for half in range(2):
                ring(1, i - 16, half).wait_recv()

        @pl.when((i >= 14) & (i < 28))
        def _():
            for half in range(2):
                ring(1, i - 14, half).start()

        @pl.when((i >= 30) & (i < 42))
        def _():
            for half in range(2):
                ring(2, i - 30, half).wait_recv()
            slot = i - 26
            dx[slot] = (dx[slot].astype(F32) + rr[i - 30].astype(F32)).astype(BF16)

        @pl.when((i >= 28) & (i < 42))
        def _():
            for half in range(2):
                ring(2, i - 28, half).start()

        @pl.when(i < 8)
        def _():
            hidden_load(i).wait()
            chunk = hidden_chunk(i)
            hrow[chunk] = ht[chunk].T

        @pl.when((i < 8) & (i % 2 == 0))
        def _():
            for j in range(2):
                for half in range(2):
                    hidden_send(i + j, half).start()

        @at(7, i)
        def _():
            @pl.loop(8, SLOTS)
            def _(slot):
                for half in range(2):
                    hidden_send(slot, half).start()

        @at(8, i)
        def _():
            wi_copy.start()
            locals_[5].wait()
            wo_copy.wait_recv()

        at(MIXED_AT, i)(mixed_task)

        @pl.when((i >= LAG) & (i < LAG + SLOTS))
        def _():
            hidden_task(i - LAG)

        for part in range(2):
            for q in range(2):
                at(GWO_AT[part][q], i)(functools.partial(weight_task, act, up, gwo, q, part))
                at(GWI_AT[part][q], i)(functools.partial(weight_task, gh, mx, gwi, q, part))

        @at(DX_FROM, i)
        def _():
            locals_[6].wait()
            wi_copy.wait_recv()

        @pl.when((i >= DX_FROM) & (i < DX_FROM + SLOTS))
        def _():
            dx_task((i - DX_FROM + 2) % SLOTS)

        for m in range(2):
            for stage in range(5):
                if RED_AT[m][stage] is not None:
                    at(RED_AT[m][stage], i)(functools.partial(reduce_stage, m, stage))
        return carry

    lax.fori_loop(0, STEPS - 2, step, 0)

    edge_copies = (
        remote(gmb.at[pl.ds(T - HALO, HALO)], gib.at[0], halo_send.at[2], halo_recv.at[2], next_dev),
        remote(gmb.at[pl.ds(0, HALO)], gib.at[1], halo_send.at[3], halo_recv.at[3], prev_dev),
    )
    sm[7:8] = jnp.zeros((1, D), F32)
    b0 = jnp.sum(bias[0], axis=0, keepdims=True)
    b1 = jnp.sum(bias[1], axis=0, keepdims=True)
    sm[7:8, 0:H] = jnp.where(xh == 0, b0, b1)
    sm[7:8, 384:384 + H] = jnp.where(xh == 0, b1, b0)
    for a in range(2):
        for half in range(2):
            ring(2, HOPS - 2 + a, half).wait_recv()
        done = up[a].astype(F32) + (dx[a].astype(F32) + rr[HOPS - 2 + a].astype(F32))
        done = done.astype(BF16)
        for half in range(2):
            start = half * 96 + a * HR
            gmb[start:start + HR] = done[half * HR:(half + 1) * HR]
            gf[HALO + start:HALO + start + HR] = done[half * HR:(half + 1) * HR].astype(F32)
        edge_copies[1 - a].start()

        @pl.loop(0, D // 128)
        def _(n):
            cols = pl.ds(pl.multiple_of(n * 128, 128), 128)
            for tap in range(KW):
                added = jnp.zeros((1, 128), F32)
                for half in range(2):
                    start = HALO + half * 96 + a * HR
                    product = gf[start:start + HR, cols] * xf[start - 3 + tap:start - 3 + tap + HR, cols]
                    added = added + jnp.sum(product, axis=0, keepdims=True)
                if a == 0:
                    sm[tap:tap + 1, cols] = added
                else:
                    sm[tap:tap + 1, cols] += added

        if a == 0:
            reduce_stage(1, 4)
            ag_core(0, 1 - c).wait_recv()
            for half in range(2):
                reduce_out(0, half).start()

    def sm_core():
        return remote(sms, smc, s_send.at[0], s_recv.at[0], core_dev)

    def sm_y(n, source):
        return remote(smy.at[source], smy.at[source], s_send.at[n], s_recv.at[n], y_dev(n))

    def sm_x(n, source, device):
        return remote(smx.at[source], smx.at[source], s_send.at[4 + n], s_recv.at[4 + n], device)

    def sm_z(n, source):
        return remote(smz.at[source], smz.at[source], s_send.at[6 + n], s_recv.at[6 + n], z_dev(n))

    def added_up(ref, count):
        total = ref[0].astype(F32)
        for n in range(1, count):
            total = total + ref[n].astype(F32)
        return total

    sms[0:8] = sm[:, 0:640].astype(BF16)
    sms[8:16] = sm[:, 640:1280].astype(BF16)
    sm_core().start()
    sm_core().wait_recv()
    smy[y] = (sms[...].astype(F32) + smc[...].astype(F32)).astype(BF16)
    for n in range(1, 4):
        sm_y(n, y).start()
    for copy in edge_copies:
        copy.wait_recv()
    gf[pl.ds(0, HALO)] = jnp.where(tp == 0, 0.0, gib[0].astype(F32))
    gf[pl.ds(T + HALO, HALO)] = jnp.where(tp == 15, 0.0, gib[1].astype(F32))
    for n in range(1, 4):
        sm_y(n, (y + 4 - n) % 4).wait_recv()
    smx[me_x] = added_up(smy, 4).astype(BF16)
    x_devices = (xl_dev, xh_dev, xd_dev)
    for n in range(3):
        sm_x(n, me_x, x_devices[n]).start()
    ag_core(1, 1 - c).wait_recv()
    for half in range(2):
        reduce_out(1, half).start()
    for n, source in enumerate((xh * 2 + 1 - xl, (1 - xh) * 2 + xl, (1 - xh) * 2 + 1 - xl)):
        sm_x(n, source, x_devices[n]).wait_recv()
    smz[z] = added_up(smx, 4).astype(BF16)
    for n in range(1, 8):
        sm_z(n, z).start()

    @pl.loop(0, D // 128)
    def _(n):
        cols = pl.ds(pl.multiple_of(n * 128, 128), 128)
        taps = k_ref[:, cols]
        out = gf[HALO:HALO + T, cols]
        for tap in range(KW):
            out = out + taps[tap:tap + 1] * gf[HALO + 3 - tap:HALO + 3 - tap + T, cols]
        gio[:, cols] = out.astype(BF16)

    gi_out = pltpu.make_async_copy(gio, gi_hbm.at[0], o_sem.at[2, 0])
    gi_out.start()

    @pl.loop(0, HOPS)
    def _(hop):
        for phase in range(3):
            for half in range(2):
                ring(phase, hop, half).wait_send()

    @pl.loop(0, SLOTS)
    def _(slot):
        for half in range(2):
            hidden_send(slot, half).wait_send()

    wo_copy.wait_send()
    wi_copy.wait_send()
    for copy in halo_copies + edge_copies:
        copy.wait_send()
    for m in range(2):
        red_core(m).wait_send()
        for n in range(1, 4):
            red_y(m, n).wait_send()
            ag_y(m, n, y).wait_send()
        for copy in red_x(m):
            copy.wait_send()
        ag_core(m, c).wait_send()
    sm_core().wait_send()
    for n in range(1, 4):
        sm_y(n, y).wait_send()
    for n in range(3):
        sm_x(n, me_x, x_devices[n]).wait_send()
    for n in range(1, 8):
        sm_z(n, z).wait_send()
    for n in range(1, 8):
        sm_z(n, (z + 8 - n) % 8).wait_recv()
    whole = added_up(smz, 8)
    row = lax.broadcasted_iota(jnp.int32, (16, 640), 0)
    whole = jnp.where(row % 8 == 7, smz[z].astype(F32), whole)
    sm_ref[:, 0:640] = whole[0:8]
    sm_ref[:, 640:1280] = whole[8:16]
    last = sm_ref[7:8, :]
    sm_ref[7:8, 0:H] = jnp.where(xh == 0, last[:, 0:H], last[:, 384:384 + H])
    gi_out.wait()
    for m in range(2):
        for half in range(2):
            reduce_out(m, half).wait()

def shards(inputs, saved_hidden, upstream, w_in, w_out, kernel):
    anyspace = pl.BlockSpec(memory_space=pl.ANY)
    vmem = pl.BlockSpec(memory_space=pltpu.VMEM)
    dma = pltpu.SemaphoreType.DMA
    grad_inputs, gwo, gwi, small = pl.pallas_call(
        body,
        out_shape=(
            jax.ShapeDtypeStruct((1, T, D), BF16),
            jax.ShapeDtypeStruct((H, D), BF16),
            jax.ShapeDtypeStruct((H, D), BF16),
            jax.ShapeDtypeStruct((8, D), F32),
        ),
        in_specs=[anyspace] * 5 + [vmem],
        out_specs=(anyspace, anyspace, anyspace, vmem),
        scratch_shapes=[
            pltpu.VMEM((SLOTS, SR, D), BF16),
            pltpu.VMEM((SLOTS, SR, D), BF16),
            pltpu.VMEM((SLOTS, SR, D), BF16),
            pltpu.VMEM((HOPS, SR, D), BF16),
            pltpu.VMEM((8, H, 2 * T), BF16),
            pltpu.VMEM((8, 2 * T, H), BF16),
            pltpu.VMEM((SLOTS, SR, H), BF16),
            pltpu.VMEM((2, SLOTS, SR, H), BF16),
            pltpu.VMEM((2, SLOTS, SR, H), BF16),
            pltpu.VMEM((2, H, D), BF16),
            pltpu.VMEM((2, H, D), BF16),
            pltpu.VMEM((2, H, D), F32),
            pltpu.VMEM((2, H, D), F32),
            pltpu.VMEM((H, 8 * SR), BF16),
            pltpu.VMEM((2, 8, H), F32),
            pltpu.VMEM((2, 2, 2, H, 640), BF16),
            pltpu.VMEM((2, 2, H, 640), BF16),
            pltpu.VMEM((2, 4, 2, 80, 640), BF16),
            pltpu.VMEM((2, 3, 2, 80, 640), BF16),
            pltpu.VMEM((2, 2, 80, 640), BF16),
            pltpu.VMEM((2, 4, 80, 640), BF16),
            pltpu.VMEM((2, 2, H, 640), BF16),
            pltpu.VMEM((T + 2 * HALO, D), BF16),
            pltpu.VMEM((T + 2 * HALO, D), F32),
            pltpu.VMEM((T + 2 * HALO, D), F32),
            pltpu.VMEM((T, D), BF16),
            pltpu.VMEM((T, D), BF16),
            pltpu.VMEM((2, HALO, D), BF16),
            pltpu.VMEM((8, D), F32),
            pltpu.VMEM((16, 640), BF16),
            pltpu.VMEM((16, 640), BF16),
            pltpu.VMEM((4, 16, 640), BF16),
            pltpu.VMEM((4, 16, 640), BF16),
            pltpu.VMEM((8, 16, 640), BF16),
            dma((3, HOPS, 2)), dma((3, HOPS, 2)),
            dma((SLOTS, 2)), dma((SLOTS, 2)), dma((8,)),
            dma((2,)), dma((2,)), dma((7,)), dma((3, 2)),
            dma((4,)), dma((4,)),
            dma((2, 11)), dma((2, 11)),
            dma((14,)), dma((14,)),
        ],
        compiler_params=pltpu.CompilerParams(
            collective_id=0, has_side_effects=True, vmem_limit_bytes=64 * 1024 * 1024 - 65536),
        name="step",
    )(inputs, jnp.swapaxes(saved_hidden, 1, 2), upstream, w_in.T, w_out, kernel)
    return grad_inputs, gwi.astype(F32).T, gwo.astype(F32), small[7, :H], small[:KW]


def solution(mesh):
    in_specs = (
        P("dp", "tp", None), P("dp", None, "tp"), P("dp", "tp", None), P(None, "tp"), P("tp", None), P())
    out_specs = (P("dp", "tp", None), P(None, "tp"), P("tp", None), P("tp"), P())
    return jax.shard_map(shards, mesh=mesh, in_specs=in_specs, out_specs=out_specs, check_vma=False)
```

```python
import functools

import jax
import jax.numpy as jnp
from jax import lax
from jax.experimental import pallas as pl
from jax.experimental.pallas import tpu as pltpu
from jax.sharding import PartitionSpec as P

KW = 7
D = 1280
H = 320
T = 192
SLOTS = 16
HR = 48
HC = D // 2
SR = 2 * HR
HOPS = SLOTS - 2
HALO = 16
MESH_ID = pl.DeviceIdType.MESH
F32 = jnp.float32
BF16 = jnp.bfloat16

LAG = 6
RELAY_AT = (4, 18)
GWO_AT = ((14, 15), (22, 23))
DX_FROM = 20
GWI_AT = (((0, 0), 25), ((1, 1), 28), ((0, 1), 30), ((1, 0), 31))
TAPS_FROM = 28
SMALL_AT = (36, 37, 39, 41)
RED_AT = ((24, 26, 32, 35, 39), (31, 32, 37, 40, None))
STEPS = 3 * HOPS + 2


def dot_nt(a, b):
    return lax.dot_general(a, b, (((1,), (1,)), ((), ())), preferred_element_type=F32)


def gelu_parts(x):
    a = jnp.abs(x) * 0.7071067811865476
    t = 1.0 / (1.0 + 0.5 * a)
    p = 0.17087277
    for coef in (
        -0.82215223,
        1.48851587,
        -1.13520398,
        0.27886807,
        -0.18628806,
        0.09678418,
        0.37409196,
        1.00002368,
        -1.26551223,
    ):
        p = p * t + coef
    square = a * a
    tail = 0.5 * t * jnp.exp(p - square)
    cdf = jnp.where(x >= 0, 1.0 - tail, tail)
    slope = cdf + x * (0.3989422804014327 * jnp.exp(-square))
    return x * cdf, slope


def body(
    x_hbm, h_hbm, u_hbm, wi_hbm, wo_hbm, k_ref,
    gm_hbm, gwo_hbm, gwi_hbm, sm_ref,
    up, xg, mx, dx, rr, ht, hrow, hh, act, gh, wo, wi, gwo, gwi, actt, bias,
    cs, cr, ys, yr, xs, xr, fout,
    xf, gx, gmb, gib, sm, sms, smc, smy, smx, smp, smz, smg,
    z_send, z_recv, h_send, h_recv, h_load, w_send, w_recv, l_sem, o_sem,
    halo_send, halo_recv, edge_send, edge_recv, red_send, red_recv, s_send, s_recv, zs_send, zs_recv, zg_send, zg_recv,
):
    dp, tp = lax.axis_index("dp"), lax.axis_index("tp")
    xl, y, c = dp // 8, (dp // 2) % 4, dp % 2
    z, xh = tp // 2, tp % 2
    me_x = xh * 2 + xl

    def z_dev(n):
        return (dp, (tp + 2 * n + 32) % 16)

    def y_dev(n):
        return (xl * 8 + ((y + n) % 4) * 2 + c, tp)

    core_dev = (dp + 1 - 2 * c, tp)
    xh_dev = (dp, tp + 1 - 2 * xh)
    xl_dev = (dp + 8 - 16 * xl, tp)
    xd_dev = (dp + 8 - 16 * xl, tp + 1 - 2 * xh)
    next_dev = (dp, (tp + 1) % 16)
    prev_dev = (dp, (tp + 15) % 16)

    def remote(src, dst, send, recv, device):
        return pltpu.make_async_remote_copy(
            src_ref=src, dst_ref=dst, send_sem=send, recv_sem=recv,
            device_id=device, device_id_type=MESH_ID,
        )

    def local_loads():
        copies = []
        n = 0
        for a in range(2):
            for half in range(2):
                copies.append(pltpu.make_async_copy(
                    u_hbm.at[0, pl.ds(half * 96 + a * HR, HR)], up.at[a, pl.ds(half * HR, HR)], l_sem.at[n]))
                n += 1
        for half in range(2):
            copies.append(pltpu.make_async_copy(
                x_hbm.at[0, :, pl.ds(half * HC, HC)], xg.at[half, 0, pl.ds(HALO, T)], l_sem.at[n]))
            n += 1
        copies.append(pltpu.make_async_copy(wo_hbm, wo.at[0], l_sem.at[n]))
        copies.append(pltpu.make_async_copy(wi_hbm, wi.at[0], l_sem.at[n + 1]))
        return copies

    def hidden_chunk(n):
        return (z + 8 + ((n + 1) // 2) * (1 - 2 * (n % 2))) % 8

    def hidden_load(n):
        chunk = hidden_chunk(n)
        cols = pl.ds(pl.multiple_of(chunk * 2 * T, 128), 2 * T)
        return pltpu.make_async_copy(h_hbm.at[0, :, cols], ht.at[chunk], h_load.at[n])

    def hidden_rows(slot, half, parity):
        s, a = slot // 2, slot % 2
        chunk = (z + (s if half else 8 - s)) % 8
        return chunk, pl.ds(pl.multiple_of(parity * T + half * 96 + a * HR, 16), HR)

    def hidden_send(slot, half):
        chunk, rows = hidden_rows(slot, half, 1 - xh)
        return remote(
            hrow.at[chunk, rows], hh.at[slot, pl.ds(half * HR, HR)],
            h_send.at[slot, half], h_recv.at[slot, half], xh_dev)

    own_half = pl.ds(c * 160, 160)
    other_half = pl.ds((1 - c) * 160, 160)

    def weight_copy(n):
        source, held = ((wo_hbm, wo), (wi_hbm, wi))[n]
        return remote(source.at[own_half], held.at[1, own_half], w_send.at[n, 0], w_recv.at[n, 0], xh_dev)

    def weight_relay(n, half):
        held = (wo, wi)[n]
        return remote(held.at[1, half], held.at[1, half], w_send.at[n, 1], w_recv.at[n, 1], core_dev)

    def edge_to(slot, half, a):
        step = 1 if half == a else 7
        return (slot + (xh if a else 1 - xh) * step) % 8

    def edge_send_copy(slot, half, a):
        rows = pl.ds(HALO + (T - HALO if a else 0), HALO)
        target = edge_to(slot, half, a)
        return remote(
            xg.at[half, slot, rows], xg.at[half, target, pl.ds(0 if a else T + HALO, HALO)],
            edge_send.at[half, a, slot], edge_recv.at[half, a, target], xh_dev)

    def edge_do(slot, half, a, act_on):
        @pl.when(edge_to(slot, half, a) != 0)
        def _():
            act_on(edge_send_copy(slot, half, a))

    def first_edge(half, a):
        cols = pl.ds(half * HC, HC)
        return remote(
            x_hbm.at[0, pl.ds(T - HALO if a else 0, HALO), cols],
            xg.at[half, 0, pl.ds(0 if a else T + HALO, HALO)],
            halo_send.at[half, a], edge_recv.at[half, a, 0], next_dev if a else prev_dev)

    def edge_arrival(slot, half, a):
        return remote(
            xg.at[half, slot, pl.ds(HALO, HALO)], xg.at[half, slot, pl.ds(0 if a else T + HALO, HALO)],
            edge_send.at[half, a, slot], edge_recv.at[half, a, slot], xh_dev)

    def ring(phase, hop, half, first=True):
        device = z_dev(-1 if half else 1)
        s, a = hop // 2, hop % 2
        if phase == 0:
            rows = pl.ds(half * HR, HR)
            src, dst = up.at[hop, rows], up.at[hop + 2, rows]
        elif phase == 1:
            rows = pl.ds(pl.multiple_of(HALO + a * SR, 16), SR)
            src, dst = xg.at[half, s, rows], xg.at[half, s + 1, rows]
        else:
            rows = pl.ds(pl.multiple_of(a * SR, 16), SR)
            src = dx.at[half, 7 if half else 1, rows] if first else rr.at[half, s - 1, rows]
            dst = rr.at[half, s, rows]
        return remote(src, dst, z_send.at[phase, hop, half], z_recv.at[phase, hop, half], device)

    locals_ = local_loads()
    for copy in locals_:
        copy.start()
    for n in range(8):
        hidden_load(n).start()
    barrier = pltpu.get_barrier_semaphore()
    peers = [z_dev(1), z_dev(-1)] + [y_dev(n) for n in range(1, 4)]
    peers += [core_dev, xl_dev, xh_dev, xd_dev, next_dev, prev_dev]
    for peer in peers:
        pl.semaphore_signal(barrier, inc=1, device_id=peer, device_id_type=MESH_ID)
    pl.semaphore_wait(barrier, len(peers))

    weight_copy(0).start()
    for half in range(2):
        locals_[4 + half].wait()
        for a in range(2):
            first_edge(half, a).start()
            edge_do(0, half, a, lambda copy: copy.start())

    sm[...] = jnp.zeros_like(sm)
    bias[...] = jnp.zeros_like(bias)

    def red_core(m):
        return remote(cs.at[m, 1 - c], cr.at[m], red_send.at[m, 0], red_recv.at[m, 0], core_dev)

    def red_y(m, n):
        return remote(ys.at[m, (y + n) % 4], yr.at[m, n - 1], red_send.at[m, n], red_recv.at[m, n], y_dev(n))

    def red_x(m):
        return (
            remote(xs.at[m, 0], xr.at[m, me_x], red_send.at[m, 4], red_recv.at[m, 4], xl_dev),
            remote(xs.at[m, 1], xr.at[m, me_x], red_send.at[m, 5], red_recv.at[m, 5], xh_dev),
            remote(xs.at[m, 1], xr.at[m, me_x], red_send.at[m, 6], red_recv.at[m, 6], xd_dev),
        )

    def red_x_wait(m):
        for sem, src_x, device in (
            (4, xh * 2 + 1 - xl, xl_dev), (5, (1 - xh) * 2 + xl, xh_dev), (6, (1 - xh) * 2 + 1 - xl, xd_dev),
        ):
            remote(xs.at[m, 0], xr.at[m, src_x], red_send.at[m, sem], red_recv.at[m, sem], device).wait_recv()

    def ag_y(m, n, source):
        return remote(
            fout.at[m, c, pl.ds(source * 80, 80)], fout.at[m, c, pl.ds(source * 80, 80)], red_send.at[m, 6 + n], red_recv.at[m, 6 + n], y_dev(n))

    def ag_core(m, half):
        return remote(fout.at[m, half], fout.at[m, half], red_send.at[m, 10], red_recv.at[m, 10], core_dev)

    totals = (gwo, gwi)

    def reduce_stage(m, stage):
        total = totals[m]
        if stage == 0:
            for q in range(2):
                for half in range(2):
                    cs[m, half, q] = total[q, :, half * 640:(half + 1) * 640].astype(BF16)
            red_core(m).start()
        elif stage == 1:
            red_core(m).wait_recv()
            own_cols = pl.ds(pl.multiple_of(c * 640, 128), 640)
            for q in range(2):
                for part in range(4):
                    rows = slice(part * 80, part * 80 + 80)
                    ys[m, part, q] = (total[q, rows, own_cols] + cr[m, q, rows].astype(F32)).astype(BF16)
            for n in range(1, 4):
                red_y(m, n).start()
        elif stage == 2:
            for n in range(1, 4):
                red_y(m, n).wait_recv()
            for q in range(2):
                part = ys[m, y, q].astype(F32)
                for n in range(3):
                    part = part + yr[m, n, q].astype(F32)
                xs[m, q] = part.astype(BF16)
            for copy in red_x(m):
                copy.start()
        elif stage == 3:
            red_x_wait(m)
            xr[m, me_x] = xs[m, 0]
            part = xr[m, 0].astype(F32)
            for n in range(1, 4):
                part = part + xr[m, n].astype(F32)
            fout[m, c, pl.ds(y * 80, 80)] = part.astype(BF16)
            for n in range(1, 4):
                ag_y(m, n, y).start()
        else:
            for n in range(1, 4):
                ag_y(m, n, (y + 4 - n) % 4).wait_recv()
            ag_core(m, c).start()

    def reduce_out(m, half):
        cols = pl.ds(half * 640, 640)
        return pltpu.make_async_copy(fout.at[m, half], (gwo_hbm, gwi_hbm)[m].at[:, cols], o_sem.at[m, half])

    def widen(slot, half):
        block = 2 * ((z + (slot if half else 8 - slot)) % 8) + xh
        xf[pl.ds(HALO, T)] = xg[half, slot, pl.ds(HALO, T)].astype(F32)
        xf[pl.ds(0, HALO)] = jnp.where(block == 0, 0.0, xg[half, slot, pl.ds(0, HALO)].astype(F32))
        xf[pl.ds(T + HALO, HALO)] = jnp.where(block == 15, 0.0, xg[half, slot, pl.ds(T + HALO, HALO)].astype(F32))

    def mixed_task(slot, half):
        for a in range(2):
            edge_arrival(slot, half, a).wait_recv()
        widen(slot, half)
        place = (8 - slot) % 8 if half else slot

        @pl.loop(0, HC // 128)
        def _(n):
            cols = pl.ds(pl.multiple_of(n * 128, 128), 128)
            taps = k_ref[:, pl.ds(pl.multiple_of(half * HC + n * 128, 128), 128)]
            out = xf[HALO:HALO + T, cols]
            for tap in range(KW):
                out = out + taps[tap:tap + 1] * xf[HALO - 3 + tap:HALO - 3 + tap + T, cols]
            mx[half, place, :, cols] = out.astype(BF16)

    def taps_task(place, own):
        for half in range(2):
            widen((8 - place) % 8 if half else place, half)
            gx[...] = dx[half, place].astype(F32)

            @pl.when(own)
            def _():
                for a in range(2):
                    for part in range(2):
                        start = part * 96 + a * HR
                        gx[start:start + HR] += up[a, part * HR:(part + 1) * HR, half * HC:(half + 1) * HC].astype(F32)

            @pl.loop(0, HC // 128)
            def _(n):
                cols = pl.ds(pl.multiple_of(n * 128, 128), 128)
                into = pl.ds(pl.multiple_of(half * HC + n * 128, 128), 128)
                grad = gx[:, cols]
                for tap in range(KW):
                    product = grad * xf[HALO - 3 + tap:HALO - 3 + tap + T, cols]
                    sm[tap:tap + 1, into] += jnp.sum(product, axis=0, keepdims=True)

    def place_order(n):
        return (n % 2) * (4 + n // 2) + (1 - n % 2) * ((4 - n // 2) % 4)

    def hidden_task(slot):
        for half in range(2):
            hidden_send(slot, half).wait_recv()
        gathered = up[slot]
        own = []
        for half in range(2):
            chunk, where = hidden_rows(slot, half, xh)
            own.append(hrow[chunk, where])
        own = jnp.concatenate(own, axis=0)
        for q in range(2):
            back = dot_nt(gathered, wo[q])
            value, slope = gelu_parts((hh[slot] if q else own).astype(F32))
            grad = (slope * back).astype(BF16)
            act[q, slot] = value.astype(BF16)
            for half in range(2):
                place = (8 - slot // 2) % 8 if half else slot // 2
                rows = pl.ds(pl.multiple_of(half * 96 + (slot % 2) * HR, 16), HR)
                gh[q, place, rows] = grad[half * HR:(half + 1) * HR]
            bias[q] += jnp.sum(grad.astype(F32).reshape(SR // 8, 8, H), axis=0)

    def out_weight_task(q, part):
        eight = pl.ds(part * 8, 8)
        actt[...] = act[q, eight].reshape(8 * SR, H).T

        @pl.loop(0, D // 256)
        def _(n):
            cols = pl.ds(pl.multiple_of(n * 256, 256), 256)
            value = jnp.dot(
                actt[...], up[eight, :, cols].reshape(8 * SR, 256), preferred_element_type=F32)
            if part == 0:
                gwo[q, :, cols] = value
            else:
                gwo[q, :, cols] += value

    def in_weight_task(half, part):
        four = pl.ds(part * 4, 4)
        for q in range(2):
            actt[...] = gh[q, four].reshape(4 * T, H).T
            for start, width in ((0, 256), (256, 256), (512, 128)):
                value = jnp.dot(
                    actt[...], mx[half, four, :, start:start + width].reshape(4 * T, width),
                    preferred_element_type=F32)
                cols = slice(half * HC + start, half * HC + start + width)
                if part == half:
                    gwi[q, :, cols] = value
                else:
                    gwi[q, :, cols] += value

    def dx_task(place):
        g0, g1 = gh[0, place], gh[1, place]
        for start, width in ((0, 256), (256, 256), (512, 128), (640, 256), (896, 256), (1152, 128)):
            cols = slice(start, start + width)
            half = start // HC
            dx[half, place, :, start - half * HC:start - half * HC + width] = (
                jnp.dot(g0, wi[0, :, cols], preferred_element_type=F32)
                + jnp.dot(g1, wi[1, :, cols], preferred_element_type=F32)
            ).astype(BF16)

    def sm_core():
        return remote(sms, smc, s_send.at[0], s_recv.at[0], core_dev)

    def sm_y(n, source):
        return remote(smy.at[source], smy.at[source], s_send.at[n], s_recv.at[n], y_dev(n))

    def sm_x(n, source, device):
        return remote(smx.at[source], smx.at[source], s_send.at[4 + n], s_recv.at[4 + n], device)

    def sm_scatter(piece, source):
        return remote(smp.at[piece], smz.at[source], zs_send.at[piece], zs_recv.at[source], (dp, 2 * piece + xh))

    def sm_gather(n, piece):
        return remote(smg.at[piece], smg.at[piece], zg_send.at[n], zg_recv.at[piece], z_dev(n))

    x_devices = (xl_dev, xh_dev, xd_dev)

    def added_up(ref, count):
        total = ref[0].astype(F32)
        for n in range(1, count):
            total = total + ref[n].astype(F32)
        return total

    def small_stage(stage):
        if stage == 0:
            b0 = jnp.sum(bias[0], axis=0, keepdims=True)
            b1 = jnp.sum(bias[1], axis=0, keepdims=True)
            sm[7:8, 0:H] = jnp.where(xh == 0, b0, b1)
            sm[7:8, 384:384 + H] = jnp.where(xh == 0, b1, b0)
            sms[0:8] = sm[:, 0:640].astype(BF16)
            sms[8:16] = sm[:, 640:1280].astype(BF16)
            sm_core().start()
        elif stage == 1:
            sm_core().wait_recv()
            smy[y] = (sms[...].astype(F32) + smc[...].astype(F32)).astype(BF16)
            for n in range(1, 4):
                sm_y(n, y).start()
        elif stage == 2:
            for n in range(1, 4):
                sm_y(n, (y + 4 - n) % 4).wait_recv()
            smx[me_x] = added_up(smy, 4).astype(BF16)
            for n in range(3):
                sm_x(n, me_x, x_devices[n]).start()
        else:
            for n, source in enumerate((xh * 2 + 1 - xl, (1 - xh) * 2 + xl, (1 - xh) * 2 + 1 - xl)):
                sm_x(n, source, x_devices[n]).wait_recv()
            total = added_up(smx, 4).astype(BF16)
            for piece in range(5):
                smp[piece] = total[:, piece * 128:piece * 128 + 128]
            for piece in range(5):
                @pl.when(z != piece)
                def _():
                    sm_scatter(piece, z).start()

    def small_gather():
        @pl.when(z < 5)
        def _():
            for n in range(1, 8):
                source = (z + n) % 8
                remote(smp.at[0], smz.at[source], zs_send.at[0], zs_recv.at[source], z_dev(n)).wait_recv()
            smz[z] = smp[z]
            smg[z] = added_up(smz, 8).astype(BF16)
            for n in range(1, 8):
                sm_gather(n, z).start()

    for n in range(4):
        locals_[n].wait()

    def at(step, i):
        return pl.when(i == step)

    def step(i, carry):
        for half in range(2):
            @pl.when((i >= 2) & (i < 16))
            def _():
                ring(0, i - 2, half).wait_recv()

            @pl.when(i < HOPS)
            def _():
                ring(0, i, half).start()

        for half in range(2):
            @pl.when((i >= 16) & (i < 30))
            def _():
                ring(1, i - 16, half).wait_recv()

            @pl.when((i >= 14) & (i < 28))
            def _():
                ring(1, i - 14, half).start()

        @pl.when((i >= 30) & (i < 42))
        def _():
            s = (i - 28) // 2
            rows = pl.ds(pl.multiple_of((i % 2) * SR, 16), SR)
            for half in range(2):
                ring(2, i - 30, half).wait_recv()
                place = 7 - s if half else s + 1
                rr[half, s - 1, rows] = (
                    rr[half, s - 1, rows].astype(F32) + dx[half, place, rows].astype(F32)).astype(BF16)
                ring(2, i - 28, half, first=False).start()

        @pl.when((i >= 28) & (i < 30))
        def _():
            for half in range(2):
                ring(2, i - 28, half).start()

        @pl.when((i >= 16) & (i < 30))
        def _():
            slot = (i - 16) // 2 + 1
            for a in range(2):
                @pl.when(i % 2 == a)
                def _():
                    for half in range(2):
                        edge_do(slot, half, a, lambda copy: copy.start())

        @pl.when(i < 8)
        def _():
            hidden_load(i).wait()
            chunk = hidden_chunk(i)
            hrow[chunk] = ht[chunk].T

        @pl.when((i < 8) & (i % 2 == 0))
        def _():
            for j in range(2):
                for half in range(2):
                    hidden_send(i + j, half).start()

        @at(7, i)
        def _():
            @pl.loop(8, SLOTS)
            def _(slot):
                for half in range(2):
                    hidden_send(slot, half).start()

        for n in range(2):
            @at(RELAY_AT[n], i)
            def _():
                weight_copy(n).wait_recv()
                weight_relay(n, own_half).start()

        @at(8, i)
        def _():
            weight_copy(1).start()

        @at(LAG, i)
        def _():
            locals_[6].wait()
            weight_relay(0, other_half).wait_recv()

        for half in range(2):
            @pl.when((i >= 18) & (i < 32) & (i % 2 == half))
            def _():
                mixed_task((i - 18) // 2, half)

            at(30 + half, i)(functools.partial(mixed_task, 7, half))

        @pl.when((i >= LAG) & (i < LAG + SLOTS))
        def _():
            hidden_task(i - LAG)

        for part in range(2):
            for q in range(2):
                at(GWO_AT[part][q], i)(functools.partial(out_weight_task, q, part))
        for which, when in GWI_AT:
            at(when, i)(functools.partial(in_weight_task, *which))

        @at(DX_FROM, i)
        def _():
            locals_[7].wait()
            weight_relay(1, other_half).wait_recv()

        @pl.when((i >= DX_FROM) & (i < DX_FROM + 8))
        def _():
            dx_task(place_order(i - DX_FROM))

        @pl.when((i >= TAPS_FROM) & (i < TAPS_FROM + 8))
        def _():
            taps_task(place_order(i - TAPS_FROM), i == TAPS_FROM)

        for stage in range(4):
            at(SMALL_AT[stage], i)(functools.partial(small_stage, stage))

        for m in range(2):
            for stage in range(5):
                if RED_AT[m][stage] is not None:
                    at(RED_AT[m][stage], i)(functools.partial(reduce_stage, m, stage))
        return carry

    lax.fori_loop(0, STEPS - 2, step, 0)

    edge_copies = (
        remote(gmb.at[pl.ds(T - HALO, HALO)], gib.at[0], halo_send.at[2, 0], halo_recv.at[0], next_dev),
        remote(gmb.at[pl.ds(0, HALO)], gib.at[1], halo_send.at[2, 1], halo_recv.at[1], prev_dev),
    )
    for a in range(2):
        rows = slice(a * SR, a * SR + SR)
        for half in range(2):
            ring(2, HOPS - 2 + a, half).wait_recv()
            cols = slice(half * HC, half * HC + HC)
            own = jnp.concatenate([up[n, a * HR:a * HR + HR, cols] for n in range(2)], axis=0).astype(F32)
            done = own + (dx[half, 0, rows].astype(F32) + rr[half, 6, rows].astype(F32))
            done = done.astype(BF16)
            gmb[rows, cols] = done
        edge_copies[1 - a].start()
    gm_out = [pltpu.make_async_copy(gmb, gm_hbm.at[pl.ds(HALO, T)], o_sem.at[2, 0])]
    gm_out[0].start()
    ag_core(0, 1 - c).wait_recv()
    for half in range(2):
        reduce_out(0, half).start()
    small_gather()
    reduce_stage(1, 4)
    for copy in edge_copies:
        copy.wait_recv()
    gib[0] = jnp.where(tp == 0, 0.0, gib[0].astype(F32)).astype(BF16)
    gib[1] = jnp.where(tp == 15, 0.0, gib[1].astype(F32)).astype(BF16)
    for n, row in enumerate((0, T + HALO)):
        gm_out.append(pltpu.make_async_copy(gib.at[n], gm_hbm.at[pl.ds(row, HALO)], o_sem.at[3, n]))
        gm_out[-1].start()
    ag_core(1, 1 - c).wait_recv()
    for half in range(2):
        reduce_out(1, half).start()

    @pl.loop(0, HOPS)
    def _(hop):
        for phase in range(3):
            for half in range(2):
                ring(phase, hop, half).wait_send()

    @pl.loop(0, SLOTS)
    def _(slot):
        for half in range(2):
            hidden_send(slot, half).wait_send()

    for n in range(2):
        weight_copy(n).wait_send()
        weight_relay(n, own_half).wait_send()
    for copy in edge_copies:
        copy.wait_send()
    for half in range(2):
        for a in range(2):
            first_edge(half, a).wait_send()

    @pl.loop(0, 8)
    def _(slot):
        for half in range(2):
            for a in range(2):
                edge_do(slot, half, a, lambda copy: copy.wait_send())

    for m in range(2):
        red_core(m).wait_send()
        for n in range(1, 4):
            red_y(m, n).wait_send()
            ag_y(m, n, y).wait_send()
        for copy in red_x(m):
            copy.wait_send()
        ag_core(m, c).wait_send()
    sm_core().wait_send()
    for n in range(1, 4):
        sm_y(n, y).wait_send()
    for n in range(3):
        sm_x(n, me_x, x_devices[n]).wait_send()
    row = lax.broadcasted_iota(jnp.int32, (16, 128), 0)
    for piece in range(5):
        @pl.when(z != piece)
        def _():
            sm_scatter(piece, z).wait_send()
            sm_gather(1, piece).wait_recv()

        whole = jnp.where(row % 8 == 7, smp[piece].astype(F32), smg[piece].astype(F32))
        sm_ref[:, piece * 128:piece * 128 + 128] = whole[0:8]
        sm_ref[:, piece * 128 + 640:piece * 128 + 768] = whole[8:16]

    @pl.when(z < 5)
    def _():
        for n in range(1, 8):
            sm_gather(n, z).wait_send()

    last = sm_ref[7:8, :]
    sm_ref[7:8, 0:H] = jnp.where(xh == 0, last[:, 0:H], last[:, 384:384 + H])
    for copy in gm_out:
        copy.wait()
    for m in range(2):
        for half in range(2):
            reduce_out(m, half).wait()

def finish(gm_hbm, gwo_hbm, gwi_hbm, sm_ref, k_ref, gi_out, gwo_out, gwi_out, taps_ref, bias_ref,
           gb, gf, gio, narrow, wide, in_sem, out_sem):
    loads, stores = [], []
    for n in range(4):
        rows = pl.ds((n % 2) * 160, 160)
        loads.append(pltpu.make_async_copy((gwo_hbm, gwi_hbm)[n // 2].at[rows], narrow.at[n], in_sem.at[n]))
        stores.append(pltpu.make_async_copy(wide.at[n], (gwo_out, gwi_out)[n // 2].at[rows], out_sem.at[n]))
        loads[n].start()
    loads.append(pltpu.make_async_copy(gm_hbm, gb, in_sem.at[4]))
    stores.append(pltpu.make_async_copy(gio, gi_out.at[0], out_sem.at[4]))
    loads[4].start()
    taps_ref[...] = sm_ref[0:KW]
    bias_ref[...] = sm_ref[KW, 0:H]
    for n in range(4):
        loads[n].wait()
        wide[n] = narrow[n].astype(F32)
        stores[n].start()
    loads[4].wait()
    gf[...] = gb[...].astype(F32)

    @pl.loop(0, D // 128)
    def _(n):
        cols = pl.ds(pl.multiple_of(n * 128, 128), 128)
        taps = k_ref[:, cols]
        out = gf[HALO:HALO + T, cols]
        for tap in range(KW):
            out = out + taps[tap:tap + 1] * gf[HALO + 3 - tap:HALO + 3 - tap + T, cols]
        gio[:, cols] = out.astype(BF16)

    stores[4].start()
    for store in stores:
        store.wait()


def shards(inputs, saved_hidden, upstream, w_in, w_out, kernel):
    anyspace = pl.BlockSpec(memory_space=pl.ANY)
    vmem = pl.BlockSpec(memory_space=pltpu.VMEM)
    dma = pltpu.SemaphoreType.DMA
    grad_mixed, gwo, gwi, small = pl.pallas_call(
        body,
        out_shape=(
            jax.ShapeDtypeStruct((T + 2 * HALO, D), BF16),
            jax.ShapeDtypeStruct((H, D), BF16),
            jax.ShapeDtypeStruct((H, D), BF16),
            jax.ShapeDtypeStruct((8, D), F32),
        ),
        in_specs=[anyspace] * 5 + [vmem],
        out_specs=(anyspace, anyspace, anyspace, vmem),
        scratch_shapes=[
            pltpu.VMEM((SLOTS, SR, D), BF16),
            pltpu.VMEM((2, 8, T + 2 * HALO, HC), BF16),
            pltpu.VMEM((2, 8, T, HC), BF16),
            pltpu.VMEM((2, 8, T, HC), BF16),
            pltpu.VMEM((2, 7, T, HC), BF16),
            pltpu.VMEM((8, H, 2 * T), BF16),
            pltpu.VMEM((8, 2 * T, H), BF16),
            pltpu.VMEM((SLOTS, SR, H), BF16),
            pltpu.VMEM((2, SLOTS, SR, H), BF16),
            pltpu.VMEM((2, 8, T, H), BF16),
            pltpu.VMEM((2, H, D), BF16),
            pltpu.VMEM((2, H, D), BF16),
            pltpu.VMEM((2, H, D), F32),
            pltpu.VMEM((2, H, D), F32),
            pltpu.VMEM((H, 8 * SR), BF16),
            pltpu.VMEM((2, 8, H), F32),
            pltpu.VMEM((2, 2, 2, H, 640), BF16),
            pltpu.VMEM((2, 2, H, 640), BF16),
            pltpu.VMEM((2, 4, 2, 80, 640), BF16),
            pltpu.VMEM((2, 3, 2, 80, 640), BF16),
            pltpu.VMEM((2, 2, 80, 640), BF16),
            pltpu.VMEM((2, 4, 80, 640), BF16),
            pltpu.VMEM((2, 2, H, 640), BF16),
            pltpu.VMEM((T + 2 * HALO, HC), F32),
            pltpu.VMEM((T, HC), F32),
            pltpu.VMEM((T, D), BF16),
            pltpu.VMEM((2, HALO, D), BF16),
            pltpu.VMEM((8, D), F32),
            pltpu.VMEM((16, 640), BF16),
            pltpu.VMEM((16, 640), BF16),
            pltpu.VMEM((4, 16, 640), BF16),
            pltpu.VMEM((4, 16, 640), BF16),
            pltpu.VMEM((5, 16, 128), BF16),
            pltpu.VMEM((8, 16, 128), BF16),
            pltpu.VMEM((5, 16, 128), BF16),
            dma((3, HOPS, 2)), dma((3, HOPS, 2)),
            dma((SLOTS, 2)), dma((SLOTS, 2)), dma((8,)),
            dma((2, 2)), dma((2, 2)), dma((8,)), dma((4, 2)),
            dma((3, 2)), dma((2,)), dma((2, 2, 8)), dma((2, 2, 8)),
            dma((2, 11)), dma((2, 11)),
            dma((7,)), dma((7,)), dma((5,)), dma((8,)), dma((8,)), dma((5,)),
        ],
        compiler_params=pltpu.CompilerParams(
            collective_id=0, has_side_effects=True, vmem_limit_bytes=64 * 1024 * 1024 - 65536),
        name="step",
    )(inputs, jnp.swapaxes(saved_hidden, 1, 2), upstream, w_in.T, w_out, kernel)
    grad_inputs, gwo, gwi, taps, bias = pl.pallas_call(
        finish,
        out_shape=(
            jax.ShapeDtypeStruct((1, T, D), BF16),
            jax.ShapeDtypeStruct((H, D), F32),
            jax.ShapeDtypeStruct((H, D), F32),
            jax.ShapeDtypeStruct((KW, D), F32),
            jax.ShapeDtypeStruct((H,), F32),
        ),
        in_specs=[anyspace] * 3 + [vmem, vmem],
        out_specs=(anyspace, anyspace, anyspace, vmem, vmem),
        scratch_shapes=[
            pltpu.VMEM((T + 2 * HALO, D), BF16),
            pltpu.VMEM((T + 2 * HALO, D), F32),
            pltpu.VMEM((T, D), BF16),
            pltpu.VMEM((4, 160, D), BF16),
            pltpu.VMEM((4, 160, D), F32),
            dma((5,)), dma((5,)),
        ],
        compiler_params=pltpu.CompilerParams(vmem_limit_bytes=64 * 1024 * 1024 - 65536),
        name="finish",
    )(grad_mixed, gwo, gwi, small, kernel)
    return grad_inputs, gwi.T, gwo, bias, taps


def solution(mesh):
    in_specs = (
        P("dp", "tp", None), P("dp", None, "tp"), P("dp", "tp", None), P(None, "tp"), P("tp", None), P())
    out_specs = (P("dp", "tp", None), P(None, "tp"), P("tp", None), P("tp"), P())
    return jax.shard_map(shards, mesh=mesh, in_specs=in_specs, out_specs=out_specs, check_vma=False)
```

```python
import functools

import jax
import jax.numpy as jnp
from jax import lax
from jax.experimental import pallas as pl
from jax.experimental.pallas import tpu as pltpu
from jax.sharding import PartitionSpec as P

KW = 7
D = 1280
H = 320
T = 192
SLOTS = 16
HR = 48
HC = D // 2
SR = 2 * HR
HOPS = SLOTS - 2
HALO = 16
MESH_ID = pl.DeviceIdType.MESH
F32 = jnp.float32
BF16 = jnp.bfloat16

LAG = 6
RELAY_AT = (4, 18)
GWO_AT = ((14, 15), (22, 23))
DX_FROM = 20
GWI_AT = (((0, 0), 25), ((1, 1), 28), ((0, 1), 30), ((1, 0), 31))
TAPS_FROM = 28
SMALL_AT = (36, 37, 39, 41)
RED_AT = ((24, 26, 32, 35, 39), (31, 33, 38, 40, None))
STEPS = 3 * HOPS + 2


def dot_nt(a, b):
    return lax.dot_general(a, b, (((1,), (1,)), ((), ())), preferred_element_type=F32)


def gelu_parts(x):
    a = jnp.abs(x) * 0.7071067811865476
    t = 1.0 / (1.0 + 0.5 * a)
    p = 0.17087277
    for coef in (
        -0.82215223,
        1.48851587,
        -1.13520398,
        0.27886807,
        -0.18628806,
        0.09678418,
        0.37409196,
        1.00002368,
        -1.26551223,
    ):
        p = p * t + coef
    square = a * a
    tail = 0.5 * t * jnp.exp(p - square)
    cdf = jnp.where(x >= 0, 1.0 - tail, tail)
    slope = cdf + x * (0.3989422804014327 * jnp.exp(-square))
    return x * cdf, slope


def body(
    x_hbm, h_hbm, u_hbm, wi_hbm, wo_hbm, k_ref,
    gm_hbm, gwo_hbm, gwi_hbm, sm_ref,
    up, xg, mx, dx, rr, ht, hrow, hh, act, gh, wo, wi, gwo, gwi, actt, bias,
    cs, cr, ys, yr, xs, xr, fout,
    xf, gx, gmb, gib, sm, sms, smc, smy, smx, smp, smz, smg,
    z_send, z_recv, h_send, h_recv, h_load, w_send, w_recv, l_sem, o_sem,
    halo_send, halo_recv, edge_send, edge_recv, red_send, red_recv, s_send, s_recv, zs_send, zs_recv, zg_send, zg_recv,
):
    dp, tp = lax.axis_index("dp"), lax.axis_index("tp")
    xl, y, c = dp // 8, (dp // 2) % 4, dp % 2
    z, xh = tp // 2, tp % 2
    me_x = xh * 2 + xl

    def z_dev(n):
        return (dp, (tp + 2 * n + 32) % 16)

    def y_dev(n):
        return (xl * 8 + ((y + n) % 4) * 2 + c, tp)

    core_dev = (dp + 1 - 2 * c, tp)
    xh_dev = (dp, tp + 1 - 2 * xh)
    xl_dev = (dp + 8 - 16 * xl, tp)
    xd_dev = (dp + 8 - 16 * xl, tp + 1 - 2 * xh)
    next_dev = (dp, (tp + 1) % 16)
    prev_dev = (dp, (tp + 15) % 16)

    def remote(src, dst, send, recv, device):
        return pltpu.make_async_remote_copy(
            src_ref=src, dst_ref=dst, send_sem=send, recv_sem=recv,
            device_id=device, device_id_type=MESH_ID,
        )

    def local_loads():
        copies = []
        n = 0
        for a in range(2):
            for half in range(2):
                copies.append(pltpu.make_async_copy(
                    u_hbm.at[0, pl.ds(half * 96 + a * HR, HR)], up.at[a, pl.ds(half * HR, HR)], l_sem.at[n]))
                n += 1
        for half in range(2):
            copies.append(pltpu.make_async_copy(
                x_hbm.at[0, :, pl.ds(half * HC, HC)], xg.at[half, 0, pl.ds(HALO, T)], l_sem.at[n]))
            n += 1
        copies.append(pltpu.make_async_copy(wo_hbm, wo.at[0], l_sem.at[n]))
        copies.append(pltpu.make_async_copy(wi_hbm, wi.at[0], l_sem.at[n + 1]))
        return copies

    def hidden_chunk(n):
        return (z + 8 + ((n + 1) // 2) * (1 - 2 * (n % 2))) % 8

    def hidden_load(n):
        chunk = hidden_chunk(n)
        cols = pl.ds(pl.multiple_of(chunk * 2 * T, 128), 2 * T)
        return pltpu.make_async_copy(h_hbm.at[0, :, cols], ht.at[chunk], h_load.at[n])

    def hidden_rows(slot, half, parity):
        s, a = slot // 2, slot % 2
        chunk = (z + (s if half else 8 - s)) % 8
        return chunk, pl.ds(pl.multiple_of(parity * T + half * 96 + a * HR, 16), HR)

    def hidden_send(slot, half):
        chunk, rows = hidden_rows(slot, half, 1 - xh)
        return remote(
            hrow.at[chunk, rows], hh.at[slot, pl.ds(half * HR, HR)],
            h_send.at[slot, half], h_recv.at[slot, half], xh_dev)

    own_half = pl.ds(c * 160, 160)
    other_half = pl.ds((1 - c) * 160, 160)

    def weight_copy(n):
        source, held = ((wo_hbm, wo), (wi_hbm, wi))[n]
        return remote(source.at[own_half], held.at[1, own_half], w_send.at[n, 0], w_recv.at[n, 0], xh_dev)

    def weight_relay(n, half):
        held = (wo, wi)[n]
        return remote(held.at[1, half], held.at[1, half], w_send.at[n, 1], w_recv.at[n, 1], core_dev)

    def edge_to(slot, half, a):
        step = 1 if half == a else 7
        return (slot + (xh if a else 1 - xh) * step) % 8

    def edge_send_copy(slot, half, a):
        rows = pl.ds(HALO + (T - HALO if a else 0), HALO)
        target = edge_to(slot, half, a)
        return remote(
            xg.at[half, slot, rows], xg.at[half, target, pl.ds(0 if a else T + HALO, HALO)],
            edge_send.at[half, a, slot], edge_recv.at[half, a, target], xh_dev)

    def edge_do(slot, half, a, act_on):
        @pl.when(edge_to(slot, half, a) != 0)
        def _():
            act_on(edge_send_copy(slot, half, a))

    def first_edge(half, a):
        cols = pl.ds(half * HC, HC)
        return remote(
            x_hbm.at[0, pl.ds(T - HALO if a else 0, HALO), cols],
            xg.at[half, 0, pl.ds(0 if a else T + HALO, HALO)],
            halo_send.at[half, a], edge_recv.at[half, a, 0], next_dev if a else prev_dev)

    def edge_arrival(slot, half, a):
        return remote(
            xg.at[half, slot, pl.ds(HALO, HALO)], xg.at[half, slot, pl.ds(0 if a else T + HALO, HALO)],
            edge_send.at[half, a, slot], edge_recv.at[half, a, slot], xh_dev)

    def ring(phase, hop, half, first=True):
        device = z_dev(-1 if half else 1)
        s, a = hop // 2, hop % 2
        if phase == 0:
            rows = pl.ds(half * HR, HR)
            src, dst = up.at[hop, rows], up.at[hop + 2, rows]
        elif phase == 1:
            rows = pl.ds(pl.multiple_of(HALO + a * SR, 16), SR)
            src, dst = xg.at[half, s, rows], xg.at[half, s + 1, rows]
        else:
            rows = pl.ds(pl.multiple_of(a * SR, 16), SR)
            src = dx.at[half, 7 if half else 1, rows] if first else rr.at[half, s - 1, rows]
            dst = rr.at[half, s, rows]
        return remote(src, dst, z_send.at[phase, hop, half], z_recv.at[phase, hop, half], device)

    locals_ = local_loads()
    for copy in locals_:
        copy.start()
    for n in range(8):
        hidden_load(n).start()
    barrier = pltpu.get_barrier_semaphore()
    peers = [z_dev(1), z_dev(-1)] + [y_dev(n) for n in range(1, 4)]
    peers += [core_dev, xl_dev, xh_dev, xd_dev, next_dev, prev_dev]
    for peer in peers:
        pl.semaphore_signal(barrier, inc=1, device_id=peer, device_id_type=MESH_ID)
    pl.semaphore_wait(barrier, len(peers))

    weight_copy(0).start()
    for half in range(2):
        locals_[4 + half].wait()
        for a in range(2):
            first_edge(half, a).start()
            edge_do(0, half, a, lambda copy: copy.start())

    sm[...] = jnp.zeros_like(sm)
    bias[...] = jnp.zeros_like(bias)

    def red_core(m):
        return remote(cs.at[m, 1 - c], cr.at[m], red_send.at[m, 0], red_recv.at[m, 0], core_dev)

    def red_y(m, n):
        return remote(ys.at[m, (y + n) % 4], yr.at[m, n - 1], red_send.at[m, n], red_recv.at[m, n], y_dev(n))

    def red_x(m):
        return (
            remote(xs.at[m, 0], xr.at[m, me_x], red_send.at[m, 4], red_recv.at[m, 4], xl_dev),
            remote(xs.at[m, 1], xr.at[m, me_x], red_send.at[m, 5], red_recv.at[m, 5], xh_dev),
            remote(xs.at[m, 1], xr.at[m, me_x], red_send.at[m, 6], red_recv.at[m, 6], xd_dev),
        )

    def red_x_wait(m):
        for sem, src_x, device in (
            (4, xh * 2 + 1 - xl, xl_dev), (5, (1 - xh) * 2 + xl, xh_dev), (6, (1 - xh) * 2 + 1 - xl, xd_dev),
        ):
            remote(xs.at[m, 0], xr.at[m, src_x], red_send.at[m, sem], red_recv.at[m, sem], device).wait_recv()

    def ag_y(m, n, source):
        return remote(
            fout.at[m, c, pl.ds(source * 80, 80)], fout.at[m, c, pl.ds(source * 80, 80)], red_send.at[m, 6 + n], red_recv.at[m, 6 + n], y_dev(n))

    def ag_core(m, half):
        return remote(fout.at[m, half], fout.at[m, half], red_send.at[m, 10], red_recv.at[m, 10], core_dev)

    totals = (gwo, gwi)

    def reduce_stage(m, stage):
        total = totals[m]
        if stage == 0:
            for q in range(2):
                for half in range(2):
                    cs[m, half, q] = total[q, :, half * 640:(half + 1) * 640].astype(BF16)
            red_core(m).start()
        elif stage == 1:
            red_core(m).wait_recv()
            own_cols = pl.ds(pl.multiple_of(c * 640, 128), 640)
            for q in range(2):
                for part in range(4):
                    rows = slice(part * 80, part * 80 + 80)
                    ys[m, part, q] = (total[q, rows, own_cols] + cr[m, q, rows].astype(F32)).astype(BF16)
            for n in range(1, 4):
                red_y(m, n).start()
        elif stage == 2:
            for n in range(1, 4):
                red_y(m, n).wait_recv()
            for q in range(2):
                part = ys[m, y, q].astype(F32)
                for n in range(3):
                    part = part + yr[m, n, q].astype(F32)
                xs[m, q] = part.astype(BF16)
            for copy in red_x(m):
                copy.start()
        elif stage == 3:
            red_x_wait(m)
            xr[m, me_x] = xs[m, 0]
            part = xr[m, 0].astype(F32)
            for n in range(1, 4):
                part = part + xr[m, n].astype(F32)
            fout[m, c, pl.ds(y * 80, 80)] = part.astype(BF16)
            for n in range(1, 4):
                ag_y(m, n, y).start()
        else:
            for n in range(1, 4):
                ag_y(m, n, (y + 4 - n) % 4).wait_recv()
            ag_core(m, c).start()

    def reduce_out(m, half):
        cols = pl.ds(half * 640, 640)
        return pltpu.make_async_copy(fout.at[m, half], (gwo_hbm, gwi_hbm)[m].at[:, cols], o_sem.at[m, half])

    def widen(slot, half):
        block = 2 * ((z + (slot if half else 8 - slot)) % 8) + xh
        xf[pl.ds(HALO, T)] = xg[half, slot, pl.ds(HALO, T)].astype(F32)
        xf[pl.ds(0, HALO)] = jnp.where(block == 0, 0.0, xg[half, slot, pl.ds(0, HALO)].astype(F32))
        xf[pl.ds(T + HALO, HALO)] = jnp.where(block == 15, 0.0, xg[half, slot, pl.ds(T + HALO, HALO)].astype(F32))

    def mixed_task(slot, half):
        for a in range(2):
            edge_arrival(slot, half, a).wait_recv()
        widen(slot, half)
        place = (8 - slot) % 8 if half else slot

        @pl.loop(0, HC // 128)
        def _(n):
            cols = pl.ds(pl.multiple_of(n * 128, 128), 128)
            taps = k_ref[:, pl.ds(pl.multiple_of(half * HC + n * 128, 128), 128)]
            out = xf[HALO:HALO + T, cols]
            for tap in range(KW):
                out = out + taps[tap:tap + 1] * xf[HALO - 3 + tap:HALO - 3 + tap + T, cols]
            mx[half, place, :, cols] = out.astype(BF16)

    def taps_task(place, own):
        for half in range(2):
            widen((8 - place) % 8 if half else place, half)
            gx[...] = dx[half, place].astype(F32)

            @pl.when(own)
            def _():
                for a in range(2):
                    for part in range(2):
                        start = part * 96 + a * HR
                        gx[start:start + HR] += up[a, part * HR:(part + 1) * HR, half * HC:(half + 1) * HC].astype(F32)

            @pl.loop(0, HC // 128)
            def _(n):
                cols = pl.ds(pl.multiple_of(n * 128, 128), 128)
                into = pl.ds(pl.multiple_of(half * HC + n * 128, 128), 128)
                grad = gx[:, cols]
                for tap in range(KW):
                    product = grad * xf[HALO - 3 + tap:HALO - 3 + tap + T, cols]
                    sm[tap:tap + 1, into] += jnp.sum(product, axis=0, keepdims=True)

    def place_order(n):
        return (n % 2) * (4 + n // 2) + (1 - n % 2) * ((4 - n // 2) % 4)

    def hidden_task(slot):
        for half in range(2):
            hidden_send(slot, half).wait_recv()
        gathered = up[slot]
        own = []
        for half in range(2):
            chunk, where = hidden_rows(slot, half, xh)
            own.append(hrow[chunk, where])
        own = jnp.concatenate(own, axis=0)
        for q in range(2):
            back = dot_nt(gathered, wo[q])
            value, slope = gelu_parts((hh[slot] if q else own).astype(F32))
            grad = (slope * back).astype(BF16)
            act[q, slot] = value.astype(BF16)
            for half in range(2):
                place = (8 - slot // 2) % 8 if half else slot // 2
                rows = pl.ds(pl.multiple_of(half * 96 + (slot % 2) * HR, 16), HR)
                gh[q, place, rows] = grad[half * HR:(half + 1) * HR]
            bias[q] += jnp.sum(grad.astype(F32).reshape(SR // 8, 8, H), axis=0)

    def out_weight_task(q, part):
        eight = pl.ds(part * 8, 8)
        actt[...] = act[q, eight].reshape(8 * SR, H).T

        @pl.loop(0, D // 256)
        def _(n):
            cols = pl.ds(pl.multiple_of(n * 256, 256), 256)
            value = jnp.dot(
                actt[...], up[eight, :, cols].reshape(8 * SR, 256), preferred_element_type=F32)
            if part == 0:
                gwo[q, :, cols] = value
            else:
                gwo[q, :, cols] += value

    def in_weight_task(half, part):
        four = pl.ds(part * 4, 4)
        for q in range(2):
            actt[...] = gh[q, four].reshape(4 * T, H).T
            for start, width in ((0, 256), (256, 256), (512, 128)):
                value = jnp.dot(
                    actt[...], mx[half, four, :, start:start + width].reshape(4 * T, width),
                    preferred_element_type=F32)
                cols = slice(half * HC + start, half * HC + start + width)
                if part == half:
                    gwi[q, :, cols] = value
                else:
                    gwi[q, :, cols] += value

    def dx_task(place):
        g0, g1 = gh[0, place], gh[1, place]
        for start, width in ((0, 256), (256, 256), (512, 128), (640, 256), (896, 256), (1152, 128)):
            cols = slice(start, start + width)
            half = start // HC
            dx[half, place, :, start - half * HC:start - half * HC + width] = (
                jnp.dot(g0, wi[0, :, cols], preferred_element_type=F32)
                + jnp.dot(g1, wi[1, :, cols], preferred_element_type=F32)
            ).astype(BF16)

    def sm_core():
        return remote(sms, smc, s_send.at[0], s_recv.at[0], core_dev)

    def sm_y(n, source):
        return remote(smy.at[source], smy.at[source], s_send.at[n], s_recv.at[n], y_dev(n))

    def sm_x(n, source, device):
        return remote(smx.at[source], smx.at[source], s_send.at[4 + n], s_recv.at[4 + n], device)

    def sm_scatter(piece, source):
        return remote(smp.at[piece], smz.at[source], zs_send.at[piece], zs_recv.at[source], (dp, 2 * piece + xh))

    def sm_gather(n, piece):
        return remote(smg.at[piece], smg.at[piece], zg_send.at[n], zg_recv.at[piece], z_dev(n))

    x_devices = (xl_dev, xh_dev, xd_dev)

    def added_up(ref, count):
        total = ref[0].astype(F32)
        for n in range(1, count):
            total = total + ref[n].astype(F32)
        return total

    def small_stage(stage):
        if stage == 0:
            b0 = jnp.sum(bias[0], axis=0, keepdims=True)
            b1 = jnp.sum(bias[1], axis=0, keepdims=True)
            sm[7:8, 0:H] = jnp.where(xh == 0, b0, b1)
            sm[7:8, 384:384 + H] = jnp.where(xh == 0, b1, b0)
            sms[0:8] = sm[:, 0:640].astype(BF16)
            sms[8:16] = sm[:, 640:1280].astype(BF16)
            sm_core().start()
        elif stage == 1:
            sm_core().wait_recv()
            smy[y] = (sms[...].astype(F32) + smc[...].astype(F32)).astype(BF16)
            for n in range(1, 4):
                sm_y(n, y).start()
        elif stage == 2:
            for n in range(1, 4):
                sm_y(n, (y + 4 - n) % 4).wait_recv()
            smx[me_x] = added_up(smy, 4).astype(BF16)
            for n in range(3):
                sm_x(n, me_x, x_devices[n]).start()
        else:
            for n, source in enumerate((xh * 2 + 1 - xl, (1 - xh) * 2 + xl, (1 - xh) * 2 + 1 - xl)):
                sm_x(n, source, x_devices[n]).wait_recv()
            total = added_up(smx, 4).astype(BF16)
            for piece in range(5):
                smp[piece] = total[:, piece * 128:piece * 128 + 128]
            for piece in range(5):
                @pl.when(z != piece)
                def _():
                    sm_scatter(piece, z).start()

    def small_gather():
        @pl.when(z < 5)
        def _():
            for n in range(1, 8):
                source = (z + n) % 8
                remote(smp.at[0], smz.at[source], zs_send.at[0], zs_recv.at[source], z_dev(n)).wait_recv()
            smz[z] = smp[z]
            smg[z] = added_up(smz, 8).astype(BF16)
            for n in range(1, 8):
                sm_gather(n, z).start()

    for n in range(4):
        locals_[n].wait()

    def at(step, i):
        return pl.when(i == step)

    def step(i, carry):
        for half in range(2):
            @pl.when((i >= 2) & (i < 16))
            def _():
                ring(0, i - 2, half).wait_recv()

            @pl.when(i < HOPS)
            def _():
                ring(0, i, half).start()

        for half in range(2):
            @pl.when((i >= 16) & (i < 30))
            def _():
                ring(1, i - 16, half).wait_recv()

            @pl.when((i >= 14) & (i < 28))
            def _():
                ring(1, i - 14, half).start()

        @pl.when((i >= 30) & (i < 42))
        def _():
            s = (i - 28) // 2
            rows = pl.ds(pl.multiple_of((i % 2) * SR, 16), SR)
            for half in range(2):
                ring(2, i - 30, half).wait_recv()
                place = 7 - s if half else s + 1
                rr[half, s - 1, rows] = (
                    rr[half, s - 1, rows].astype(F32) + dx[half, place, rows].astype(F32)).astype(BF16)
                ring(2, i - 28, half, first=False).start()

        @pl.when((i >= 28) & (i < 30))
        def _():
            for half in range(2):
                ring(2, i - 28, half).start()

        @pl.when((i >= 16) & (i < 30))
        def _():
            slot = (i - 16) // 2 + 1
            for a in range(2):
                @pl.when(i % 2 == a)
                def _():
                    for half in range(2):
                        edge_do(slot, half, a, lambda copy: copy.start())

        @pl.when(i < 8)
        def _():
            hidden_load(i).wait()
            chunk = hidden_chunk(i)
            hrow[chunk] = ht[chunk].T

        @pl.when((i < 8) & (i % 2 == 0))
        def _():
            for j in range(2):
                for half in range(2):
                    hidden_send(i + j, half).start()

        @at(7, i)
        def _():
            @pl.loop(8, SLOTS)
            def _(slot):
                for half in range(2):
                    hidden_send(slot, half).start()

        for n in range(2):
            @at(RELAY_AT[n], i)
            def _():
                weight_copy(n).wait_recv()
                weight_relay(n, own_half).start()

        @at(8, i)
        def _():
            weight_copy(1).start()

        @at(LAG, i)
        def _():
            locals_[6].wait()
            weight_relay(0, other_half).wait_recv()

        for half in range(2):
            @pl.when((i >= 18) & (i < 32) & (i % 2 == half))
            def _():
                mixed_task((i - 18) // 2, half)

            at(30 + half, i)(functools.partial(mixed_task, 7, half))

        @pl.when((i >= LAG) & (i < LAG + SLOTS))
        def _():
            hidden_task(i - LAG)

        for part in range(2):
            for q in range(2):
                at(GWO_AT[part][q], i)(functools.partial(out_weight_task, q, part))
        for which, when in GWI_AT:
            at(when, i)(functools.partial(in_weight_task, *which))

        @at(DX_FROM, i)
        def _():
            locals_[7].wait()
            weight_relay(1, other_half).wait_recv()

        @pl.when((i >= DX_FROM) & (i < DX_FROM + 8))
        def _():
            dx_task(place_order(i - DX_FROM))

        @pl.when((i >= TAPS_FROM) & (i < TAPS_FROM + 8))
        def _():
            taps_task(place_order(i - TAPS_FROM), i == TAPS_FROM)

        for stage in range(4):
            at(SMALL_AT[stage], i)(functools.partial(small_stage, stage))

        for m in range(2):
            for stage in range(5):
                if RED_AT[m][stage] is not None:
                    at(RED_AT[m][stage], i)(functools.partial(reduce_stage, m, stage))
        return carry

    lax.fori_loop(0, STEPS - 2, step, 0)

    edge_copies = (
        remote(gmb.at[pl.ds(T - HALO, HALO)], gib.at[0], halo_send.at[2, 0], halo_recv.at[0], next_dev),
        remote(gmb.at[pl.ds(0, HALO)], gib.at[1], halo_send.at[2, 1], halo_recv.at[1], prev_dev),
    )
    for a in range(2):
        rows = slice(a * SR, a * SR + SR)
        for half in range(2):
            ring(2, HOPS - 2 + a, half).wait_recv()
            cols = slice(half * HC, half * HC + HC)
            own = jnp.concatenate([up[n, a * HR:a * HR + HR, cols] for n in range(2)], axis=0).astype(F32)
            done = own + (dx[half, 0, rows].astype(F32) + rr[half, 6, rows].astype(F32))
            done = done.astype(BF16)
            gmb[rows, cols] = done
        edge_copies[1 - a].start()
    gm_out = [pltpu.make_async_copy(gmb, gm_hbm.at[pl.ds(HALO, T)], o_sem.at[2, 0])]
    gm_out[0].start()
    ag_core(0, 1 - c).wait_recv()
    for half in range(2):
        reduce_out(0, half).start()
    small_gather()
    reduce_stage(1, 4)
    for copy in edge_copies:
        copy.wait_recv()
    gib[0] = jnp.where(tp == 0, 0.0, gib[0].astype(F32)).astype(BF16)
    gib[1] = jnp.where(tp == 15, 0.0, gib[1].astype(F32)).astype(BF16)
    for n, row in enumerate((0, T + HALO)):
        gm_out.append(pltpu.make_async_copy(gib.at[n], gm_hbm.at[pl.ds(row, HALO)], o_sem.at[3, n]))
        gm_out[-1].start()
    ag_core(1, 1 - c).wait_recv()
    for half in range(2):
        reduce_out(1, half).start()

    @pl.loop(0, HOPS)
    def _(hop):
        for phase in range(3):
            for half in range(2):
                ring(phase, hop, half).wait_send()

    @pl.loop(0, SLOTS)
    def _(slot):
        for half in range(2):
            hidden_send(slot, half).wait_send()

    for n in range(2):
        weight_copy(n).wait_send()
        weight_relay(n, own_half).wait_send()
    for copy in edge_copies:
        copy.wait_send()
    for half in range(2):
        for a in range(2):
            first_edge(half, a).wait_send()

    @pl.loop(0, 8)
    def _(slot):
        for half in range(2):
            for a in range(2):
                edge_do(slot, half, a, lambda copy: copy.wait_send())

    for m in range(2):
        red_core(m).wait_send()
        for n in range(1, 4):
            red_y(m, n).wait_send()
            ag_y(m, n, y).wait_send()
        for copy in red_x(m):
            copy.wait_send()
        ag_core(m, c).wait_send()
    sm_core().wait_send()
    for n in range(1, 4):
        sm_y(n, y).wait_send()
    for n in range(3):
        sm_x(n, me_x, x_devices[n]).wait_send()
    row = lax.broadcasted_iota(jnp.int32, (16, 128), 0)
    for piece in range(5):
        @pl.when(z != piece)
        def _():
            sm_scatter(piece, z).wait_send()
            sm_gather(1, piece).wait_recv()

        whole = jnp.where(row % 8 == 7, smp[piece].astype(F32), smg[piece].astype(F32))
        sm_ref[:, piece * 128:piece * 128 + 128] = whole[0:8]
        sm_ref[:, piece * 128 + 640:piece * 128 + 768] = whole[8:16]

    @pl.when(z < 5)
    def _():
        for n in range(1, 8):
            sm_gather(n, z).wait_send()

    last = sm_ref[7:8, :]
    sm_ref[7:8, 0:H] = jnp.where(xh == 0, last[:, 0:H], last[:, 384:384 + H])
    for copy in gm_out:
        copy.wait()
    for m in range(2):
        for half in range(2):
            reduce_out(m, half).wait()

def finish(gm_hbm, gwo_hbm, gwi_hbm, sm_ref, k_ref, gi_out, gwo_out, gwi_out, taps_ref, bias_ref,
           gb, gf, gio, narrow, wide, in_sem, out_sem):
    loads, stores = [], []
    for n in range(4):
        rows = pl.ds((n % 2) * 160, 160)
        loads.append(pltpu.make_async_copy((gwo_hbm, gwi_hbm)[n // 2].at[rows], narrow.at[n], in_sem.at[n]))
        stores.append(pltpu.make_async_copy(wide.at[n], (gwo_out, gwi_out)[n // 2].at[rows], out_sem.at[n]))
        loads[n].start()
    loads.append(pltpu.make_async_copy(gm_hbm, gb, in_sem.at[4]))
    stores.append(pltpu.make_async_copy(gio, gi_out.at[0], out_sem.at[4]))
    loads[4].start()
    taps_ref[...] = sm_ref[0:KW]
    bias_ref[...] = sm_ref[KW, 0:H]
    for n in range(4):
        loads[n].wait()
        wide[n] = narrow[n].astype(F32)
        stores[n].start()
    loads[4].wait()
    gf[...] = gb[...].astype(F32)

    @pl.loop(0, D // 128)
    def _(n):
        cols = pl.ds(pl.multiple_of(n * 128, 128), 128)
        taps = k_ref[:, cols]
        out = gf[HALO:HALO + T, cols]
        for tap in range(KW):
            out = out + taps[tap:tap + 1] * gf[HALO + 3 - tap:HALO + 3 - tap + T, cols]
        gio[:, cols] = out.astype(BF16)

    stores[4].start()
    for store in stores:
        store.wait()


def shards(inputs, saved_hidden, upstream, w_in, w_out, kernel):
    anyspace = pl.BlockSpec(memory_space=pl.ANY)
    vmem = pl.BlockSpec(memory_space=pltpu.VMEM)
    dma = pltpu.SemaphoreType.DMA
    grad_mixed, gwo, gwi, small = pl.pallas_call(
        body,
        out_shape=(
            jax.ShapeDtypeStruct((T + 2 * HALO, D), BF16),
            jax.ShapeDtypeStruct((H, D), BF16),
            jax.ShapeDtypeStruct((H, D), BF16),
            jax.ShapeDtypeStruct((8, D), F32),
        ),
        in_specs=[anyspace] * 5 + [vmem],
        out_specs=(anyspace, anyspace, anyspace, vmem),
        scratch_shapes=[
            pltpu.VMEM((SLOTS, SR, D), BF16),
            pltpu.VMEM((2, 8, T + 2 * HALO, HC), BF16),
            pltpu.VMEM((2, 8, T, HC), BF16),
            pltpu.VMEM((2, 8, T, HC), BF16),
            pltpu.VMEM((2, 7, T, HC), BF16),
            pltpu.VMEM((8, H, 2 * T), BF16),
            pltpu.VMEM((8, 2 * T, H), BF16),
            pltpu.VMEM((SLOTS, SR, H), BF16),
            pltpu.VMEM((2, SLOTS, SR, H), BF16),
            pltpu.VMEM((2, 8, T, H), BF16),
            pltpu.VMEM((2, H, D), BF16),
            pltpu.VMEM((2, H, D), BF16),
            pltpu.VMEM((2, H, D), F32),
            pltpu.VMEM((2, H, D), F32),
            pltpu.VMEM((H, 8 * SR), BF16),
            pltpu.VMEM((2, 8, H), F32),
            pltpu.VMEM((2, 2, 2, H, 640), BF16),
            pltpu.VMEM((2, 2, H, 640), BF16),
            pltpu.VMEM((2, 4, 2, 80, 640), BF16),
            pltpu.VMEM((2, 3, 2, 80, 640), BF16),
            pltpu.VMEM((2, 2, 80, 640), BF16),
            pltpu.VMEM((2, 4, 80, 640), BF16),
            pltpu.VMEM((2, 2, H, 640), BF16),
            pltpu.VMEM((T + 2 * HALO, HC), F32),
            pltpu.VMEM((T, HC), F32),
            pltpu.VMEM((T, D), BF16),
            pltpu.VMEM((2, HALO, D), BF16),
            pltpu.VMEM((8, D), F32),
            pltpu.VMEM((16, 640), BF16),
            pltpu.VMEM((16, 640), BF16),
            pltpu.VMEM((4, 16, 640), BF16),
            pltpu.VMEM((4, 16, 640), BF16),
            pltpu.VMEM((5, 16, 128), BF16),
            pltpu.VMEM((8, 16, 128), BF16),
            pltpu.VMEM((5, 16, 128), BF16),
            dma((3, HOPS, 2)), dma((3, HOPS, 2)),
            dma((SLOTS, 2)), dma((SLOTS, 2)), dma((8,)),
            dma((2, 2)), dma((2, 2)), dma((8,)), dma((4, 2)),
            dma((3, 2)), dma((2,)), dma((2, 2, 8)), dma((2, 2, 8)),
            dma((2, 11)), dma((2, 11)),
            dma((7,)), dma((7,)), dma((5,)), dma((8,)), dma((8,)), dma((5,)),
        ],
        compiler_params=pltpu.CompilerParams(
            collective_id=0, has_side_effects=True, vmem_limit_bytes=64 * 1024 * 1024 - 65536),
        name="step",
    )(inputs, jnp.swapaxes(saved_hidden, 1, 2), upstream, w_in.T, w_out, kernel)
    grad_inputs, gwo, gwi, taps, bias = pl.pallas_call(
        finish,
        out_shape=(
            jax.ShapeDtypeStruct((1, T, D), BF16),
            jax.ShapeDtypeStruct((H, D), F32),
            jax.ShapeDtypeStruct((H, D), F32),
            jax.ShapeDtypeStruct((KW, D), F32),
            jax.ShapeDtypeStruct((H,), F32),
        ),
        in_specs=[anyspace] * 3 + [vmem, vmem],
        out_specs=(anyspace, anyspace, anyspace, vmem, vmem),
        scratch_shapes=[
            pltpu.VMEM((T + 2 * HALO, D), BF16),
            pltpu.VMEM((T + 2 * HALO, D), F32),
            pltpu.VMEM((T, D), BF16),
            pltpu.VMEM((4, 160, D), BF16),
            pltpu.VMEM((4, 160, D), F32),
            dma((5,)), dma((5,)),
        ],
        compiler_params=pltpu.CompilerParams(vmem_limit_bytes=64 * 1024 * 1024 - 65536),
        name="finish",
    )(grad_mixed, gwo, gwi, small, kernel)
    return grad_inputs, gwi.T, gwo, bias, taps


def solution(mesh):
    in_specs = (
        P("dp", "tp", None), P("dp", None, "tp"), P("dp", "tp", None), P(None, "tp"), P("tp", None), P())
    out_specs = (P("dp", "tp", None), P(None, "tp"), P("tp", None), P("tp"), P())
    return jax.shard_map(shards, mesh=mesh, in_specs=in_specs, out_specs=out_specs, check_vma=False)
```
